256 devices in a mesh: seq: 128 (over y, x_hi, z, core), head: 2 (over x_lo).
Axes of the slice: x: 4 (x_hi: 2, x_lo: 2; x = x_hi * 2 + x_lo), y: 4, z: 8, core: 2. Of those that a mesh axis runs over, the one named last changes fastest.
Arguments:
- query: bfloat16 [32768, 2048], P('seq', 'head'), may hold values from -4.5 to 4.5
- key_value: bfloat16 [32768, 512], P('seq'), may hold values from -4.5 to 4.5
- out_grad: bfloat16 [32768, 2048], P('seq', 'head'), may hold values from -48 to 48
- inputs_normed: bfloat16 [32768, 4096], P('seq'), may hold values from -24 to 24
- kv_weight: bfloat16 [2, 4096, 256], P(None, 'head'), may hold values from -0.09375 to 0.09375
- segment_ids: int32 [32768], replicated, may hold values from 0 to 7, never falling along the last dimension, each value on 1 to 8192 neighbouring positions
Outputs:
- query_grad: bfloat16 [32768, 2048], P('seq', 'head')
- input_grad: bfloat16 [32768, 4096], P('seq', 'head')
- weight_grad: float32 [2, 4096, 256], P('head', 'seq')
The draws below stay inside these ranges and needn't reach their ends.
All inputs are finite; a program needn't handle non-finite values.
Results may differ from the reference program's by a relative error of at most 0.015.
Values may be sent and summed in bfloat16 or wider, within the bound.
No kernel may reach another device: no remote copies, remote signals or barrier semaphores. Data moves between devices by JAX's collectives and lax.ppermute only.
A program may use at most 64 MiB of HBM per device.

```python
import math
import jax
import jax.numpy as jnp
import numpy as np
from jax import lax

D = 4096
H = 8
HD = 256
WIN = 2048
TOK_DEV = 256
TOKENS = 32768


def draw_query(key, part):
    base_draw = jnp.clip(jax.random.normal(jax.random.fold_in(key, 13), (TOKENS, H * HD)), -4.5, 4.5)
    return base_draw.astype(jnp.bfloat16)


def draw_key_value(key, part):
    key_part = jnp.clip(jax.random.normal(jax.random.fold_in(key, 11), (TOKENS, HD)), -4.5, 4.5)
    value_part = jnp.clip(jax.random.normal(jax.random.fold_in(key, 12), (TOKENS, HD)), -4.5, 4.5)
    return jnp.concatenate([key_part, value_part], axis=1).astype(jnp.bfloat16)


def with_spikes(values, rng, source, target, blocks, factor):
    owner, partner = [(jnp.arange(values.shape[dim]) // (values.shape[dim] // blocks)).reshape([-1 if axis == dim else 1 for axis in range(values.ndim)]) for dim in (source, target)]
    chosen = jax.random.permutation(rng, blocks)[partner]
    strong = (owner == chosen) | (owner == (partner + blocks // 2) % blocks)
    return jnp.where(strong, factor * values, values)


def level_of(rng, shape, cuts, smallest, largest):
    factor_of = 1.0
    for position, parts in cuts:
        steps = jax.random.uniform(jax.random.fold_in(jax.random.fold_in(rng, 6), position), (parts,), jnp.float32, smallest / len(cuts), largest / len(cuts))
        factor_of = factor_of * jnp.repeat(jnp.exp(steps), shape[position] // parts).reshape((-1,) + (1,) * (len(shape) - 1 - position))
    return factor_of


def split_up(number_of, total, limit, skew):
    loads = [(1 << 20) // math.isqrt(rank ** skew) + 1 for rank in range(2, number_of + 1)]
    spare, counts = total - limit - (number_of - 1), [1] * (number_of - 1)
    while spare > 0:
        free = [i for i in range(number_of - 1) if counts[i] < limit]
        whole, left = sum([loads[i] for i in free]), spare
        for i in free:
            addition = min(limit - counts[i], max(1, left * loads[i] // whole), spare)
            counts[i] = counts[i] + addition
            spare = spare - addition
    return np.array([limit] + counts)


def ragged_sizes(own_key, count, total, reach, lean):
    if count == 2:
        one = jax.random.randint(own_key, (), max(1, total - reach), min(reach, total - 1) + 1)
        return jnp.stack([one, total - one])
    sizes = jnp.asarray(split_up(count, total, reach, lean), jnp.int32)
    twos = (count - 1) // 2
    giver, taker = sizes[1:1 + 2 * twos:2], sizes[2:2 + 2 * twos:2]
    room = jnp.minimum(giver - 1, reach - taker)
    passed = jax.random.randint(jax.random.fold_in(own_key, 1), (twos,), 0, 1 << 20) % (room + 1)
    sizes = sizes.at[1:1 + 2 * twos:2].set(giver - passed).at[2:2 + 2 * twos:2].set(taker + passed)
    return sizes[jax.random.permutation(jax.random.fold_in(own_key, 2), count)]


def normal_values(own_key, extent, scale, reach, pieces=(), kind=jnp.bfloat16):
    level = level_of(own_key, extent, pieces, -0.22, 0.18) if pieces else 1.0
    entries = jax.random.normal(own_key, extent, jnp.float32) * scale * level
    return jnp.minimum(jnp.maximum(entries, -reach), reach).astype(kind)


def noise_with(key, dims, width, most, cuts, heavy, kind=jnp.bfloat16):
    drawn = width * jax.random.normal(key, dims, jnp.float32)
    if cuts:
        drawn = drawn * level_of(key, dims, cuts, -0.22, 0.18)
    return jnp.clip(with_spikes(drawn, jax.random.fold_in(key, 3), *heavy), -most, most).astype(kind)


def setup_inputs(seed: int = 0) -> dict:
    key_of = jax.random.split(jax.random.key(seed), 7)
    return {
        "query": draw_query(jax.random.fold_in(key_of[6], 71), 0),
        "key_value": draw_key_value(jax.random.fold_in(key_of[6], 71), 0),
        "out_grad": normal_values(key_of[2], (TOKENS, H * HD), 8.0, 48.0, ((0, 128), (1, 2))),
        "inputs_normed": noise_with(key_of[3], (TOKENS, D), 1.0, 24.0, ((0, 128),), (0, 1, 128, 5.5)),
        "kv_weight": normal_values(key_of[4], (2, D, HD), D ** -0.5, 0.09375, ((1, 2),)),
        "segment_ids": jnp.searchsorted(jnp.cumsum(ragged_sizes(key_of[5], max(3, TOKENS // (2 * WIN)), TOKENS, min(4 * WIN, TOKENS - WIN), 1)), jnp.arange(TOKENS), side="right").astype(jnp.int32),
    }


def attention_block(query_rows, out_rows, window, allowed, head_count):
    head_dim = window.shape[1] // 2
    tok_rows = query_rows.shape[0]
    inv_root = 1.0 / math.sqrt(head_dim)
    key_rows = window[:, :head_dim]
    value_rows = window[:, head_dim:]
    flat_q = query_rows.reshape(tok_rows * head_count, head_dim)
    flat_do = out_rows.reshape(tok_rows * head_count, head_dim)
    scores = jnp.dot(flat_q, key_rows.T, preferred_element_type=jnp.float32) * inv_root
    scores = scores.reshape(tok_rows, head_count, -1)
    masked = jnp.where(allowed[:, None, :], scores, -jnp.inf)
    row_max = lax.optimization_barrier(jnp.max(masked, axis=-1, keepdims=True))
    shifted = jnp.exp(masked - row_max)
    probabilities = (shifted / lax.optimization_barrier(jnp.sum(shifted, axis=-1, keepdims=True))).reshape(tok_rows * head_count, -1)
    prob_bf16 = probabilities.astype(jnp.bfloat16)
    attended = jnp.dot(prob_bf16, value_rows, preferred_element_type=jnp.float32)
    row_delta = lax.optimization_barrier(jnp.sum(flat_do.astype(jnp.float32) * attended, axis=-1, keepdims=True))
    prob_grad = jnp.dot(flat_do, value_rows.T, preferred_element_type=jnp.float32)
    dscore_b = (probabilities * (prob_grad - row_delta)).astype(jnp.bfloat16)
    query_grad = (jnp.dot(dscore_b, key_rows, preferred_element_type=jnp.float32) * inv_root).astype(jnp.bfloat16)
    query_grad = query_grad.reshape(tok_rows, head_count * head_dim)
    key_grad = jnp.dot(dscore_b.T, flat_q, preferred_element_type=jnp.float32) * inv_root
    value_grad = jnp.dot(prob_bf16.T, flat_do, preferred_element_type=jnp.float32)
    return (query_grad, jnp.concatenate([key_grad, value_grad], axis=1))

def reference(query, key_value, out_grad, inputs_normed, kv_weight, segment_ids):
    tok_rows = TOK_DEV
    span = WIN + tok_rows
    block_count = TOKENS // tok_rows
    padded_kv = jnp.concatenate([jnp.zeros((WIN, 2 * HD), key_value.dtype), key_value], axis=0)
    padded_seg = jnp.concatenate([jnp.full((WIN,), -1, jnp.int32), segment_ids.astype(jnp.int32)], axis=0)

    def one_block(accumulated, block_index):
        begin_row = (block_index * tok_rows).astype(jnp.int32)
        window = lax.dynamic_slice_in_dim(padded_kv, begin_row, span, 0)
        key_seg = lax.dynamic_slice_in_dim(padded_seg, begin_row, span, 0)
        query_seg = lax.dynamic_slice_in_dim(segment_ids.astype(jnp.int32), begin_row, tok_rows, 0)
        query_pos = begin_row + jnp.arange(tok_rows, dtype=jnp.int32)
        key_pos = begin_row - WIN + jnp.arange(span, dtype=jnp.int32)
        distance = query_pos[:, None] - key_pos[None, :]
        allowed = (distance >= 0) & (distance < WIN) & (query_seg[:, None] == key_seg[None, :])
        query_rows = lax.dynamic_slice_in_dim(query, begin_row, tok_rows, 0)
        out_rows = lax.dynamic_slice_in_dim(out_grad, begin_row, tok_rows, 0)
        query_grad, window_grad = attention_block(query_rows, out_rows, window, allowed, H)
        old_part = lax.dynamic_slice_in_dim(accumulated, begin_row, span, 0)
        accumulated = lax.dynamic_update_slice_in_dim(accumulated, old_part + window_grad, begin_row, 0)
        return (accumulated, query_grad)
    start_sum = jnp.zeros((WIN + TOKENS, 2 * HD), jnp.float32)
    accumulated, query_blocks = lax.scan(one_block, start_sum, jnp.arange(block_count, dtype=jnp.int32))
    query_grad = query_blocks.reshape(TOKENS, H * HD)
    kv_grad = accumulated[WIN:].astype(jnp.bfloat16)
    stacked_weight = jnp.concatenate([kv_weight[0], kv_weight[1]], axis=1)
    input_grad = jnp.dot(kv_grad, stacked_weight.T, preferred_element_type=jnp.float32).astype(jnp.bfloat16)
    norm_factor = 1.0 / math.sqrt(TOKENS)
    key_weight = jnp.dot(inputs_normed.T, kv_grad[:, :HD], preferred_element_type=jnp.float32) * norm_factor
    value_weight = jnp.dot(inputs_normed.T, kv_grad[:, HD:], preferred_element_type=jnp.float32) * norm_factor
    weight_grad = jnp.stack([key_weight, value_weight], axis=0)
    return (query_grad, input_grad, weight_grad)
```

```python
import math

import jax
import jax.numpy as jnp
from jax import lax
from jax.sharding import Mesh
from jax.sharding import PartitionSpec as P

WIN = 2048
SEQ = ("y", "xh", "z", "c")
ALL = ("y", "xh", "z", "c", "l")
PAIRS = 64
LINE = 8
BF = jnp.bfloat16
F32 = jnp.float32


def moved(value, steps, flip):
    routes = []
    for source in range(PAIRS):
        target = source + steps
        if not 0 <= target < PAIRS:
            continue
        turn = int(flip and source // LINE != target // LINE)
        for core in range(2):
            for side in range(2):
                routes.append(((source * 2 + core) * 2 + side, (target * 2 + core) * 2 + (side ^ turn)))
    return lax.ppermute(value, ALL, routes)


def swapped(value, axis):
    return lax.ppermute(value, axis, [(0, 1), (1, 0)])


def turned(value, axis, steps):
    count = lax.axis_size(axis)
    return lax.ppermute(value, axis, [(i, (i + steps) % count) for i in range(count)])


def columns(value, which, width):
    return lax.dynamic_slice_in_dim(value, which * width, width, 1)


def attention_block(query_rows, out_rows, key_rows, value_rows, allowed, head_count):
    head_dim = key_rows.shape[1]
    tok_rows = query_rows.shape[0]
    inv_root = 1.0 / math.sqrt(head_dim)
    flat_q = query_rows.reshape(tok_rows * head_count, head_dim)
    flat_do = out_rows.reshape(tok_rows * head_count, head_dim)
    scores = jnp.dot(flat_q, key_rows.T, preferred_element_type=F32) * inv_root
    scores = scores.reshape(tok_rows, head_count, -1)
    masked = jnp.where(allowed[:, None, :], scores, -jnp.inf)
    row_max = jnp.max(masked, axis=-1, keepdims=True)
    shifted = jnp.exp(masked - row_max)
    probabilities = (shifted / jnp.sum(shifted, axis=-1, keepdims=True)).reshape(
        tok_rows * head_count, -1
    )
    prob_bf16 = probabilities.astype(BF)
    attended = jnp.dot(prob_bf16, value_rows, preferred_element_type=F32)
    row_delta = jnp.sum(flat_do.astype(F32) * attended, axis=-1, keepdims=True)
    prob_grad = jnp.dot(flat_do, value_rows.T, preferred_element_type=F32)
    dscore_b = (probabilities * (prob_grad - row_delta)).astype(BF)
    query_grad = (jnp.dot(dscore_b, key_rows, preferred_element_type=F32) * inv_root).astype(BF)
    query_grad = query_grad.reshape(tok_rows, head_count * head_dim)
    key_grad = jnp.dot(dscore_b.T, flat_q, preferred_element_type=F32) * inv_root
    value_grad = jnp.dot(prob_bf16.T, flat_do, preferred_element_type=F32)
    return query_grad, jnp.concatenate([key_grad, value_grad], axis=1).astype(BF)


def local(query, key_value, out_grad, inputs_normed, kv_weight, segment_ids):
    tok = query.shape[0]
    hd = key_value.shape[1] // 2
    heads = query.shape[1] // hd
    y, xh, z, c, l = (lax.axis_index(axis) for axis in ALL)
    seq_index = lax.axis_index(SEQ)

    def taken(distance):
        turn = (z + distance >= LINE).astype(jnp.int32)
        return columns(key_value, l ^ turn, hd)

    mine = {4: moved(taken(4), 4, True), 2: moved(taken(2), 2, True), 1: moved(taken(1), 1, True)}
    mine[3] = moved(mine[2], 1, False)
    blocks = {0: key_value}
    for d in (1, 2, 3, 4):
        other = swapped(mine[d], "l")
        blocks[d] = jnp.where(
            l == 0,
            jnp.concatenate([mine[d], other], axis=1),
            jnp.concatenate([other, mine[d]], axis=1),
        )
    near = swapped(
        jnp.where(
            c == 0,
            jnp.concatenate([blocks[1], blocks[0]], axis=0),
            jnp.concatenate([blocks[2], blocks[1]], axis=0),
        ),
        "c",
    )
    far = swapped(
        jnp.where(
            c == 0,
            jnp.concatenate([blocks[3], blocks[2]], axis=0),
            jnp.concatenate([blocks[4], blocks[3]], axis=0),
        ),
        "c",
    )
    width = inputs_normed.shape[1] // 4
    x_parts = [columns(inputs_normed, y, width)]
    for k in (1, 2, 3):
        x_parts.append(turned(columns(inputs_normed, (y + k) % 4, width), "y", k))
    x_rows = jnp.concatenate(x_parts, axis=0)

    window = jnp.concatenate([blocks[d] for d in (4, 3, 2, 1, 0)] + [far, near], axis=0)
    window, x_rows = lax.optimization_barrier((window, x_rows))
    order = jnp.array([0, 2, 4, 6, 8, 1, 3, 5, 7], jnp.int32)
    begin = seq_index * tok
    padded = jnp.concatenate([jnp.full((WIN,), -1, jnp.int32), segment_ids], axis=0)
    natural = lax.dynamic_slice_in_dim(padded, begin, WIN + tok, 0).reshape(9, tok)
    key_seg = jnp.concatenate([natural[i] for i in (0, 2, 4, 6, 8, 1, 3, 5, 7)], axis=0)
    query_seg = natural[8]
    key_pos = (order[:, None] * tok + jnp.arange(tok, dtype=jnp.int32)[None, :]).reshape(-1)
    distance = WIN + jnp.arange(tok, dtype=jnp.int32)[:, None] - key_pos[None, :]
    allowed = (distance >= 0) & (distance < WIN) & (query_seg[:, None] == key_seg[None, :])
    query_grad, grads = attention_block(
        query, out_grad, window[:, :hd], window[:, hd:], allowed, heads
    )

    arrived = swapped(grads[5 * tok :], "c")
    empty = jnp.zeros((tok, 2 * hd), BF)
    shifted = lax.dynamic_slice_in_dim(
        jnp.concatenate([empty, arrived, empty], axis=0), c * tok, 5 * tok, 0
    )
    core_sum = grads[: 5 * tok].astype(F32) + shifted.astype(F32)
    limit = {4: z < 4, 3: (z + LINE - 1) % LINE < 2, 2: z < 2, 1: z < 1, 0: z < 0}
    sums = {}
    for d in (4, 3, 2, 1, 0):
        part = core_sum[(4 - d) * tok : (5 - d) * tok]
        side = l ^ limit[d].astype(jnp.int32)
        got = swapped(columns(part, 1 - side, hd).astype(BF), "l")
        sums[d] = columns(part, side, hd) + got.astype(F32)
    from_four = moved(sums[4].astype(BF), -4, True)
    from_three = moved(sums[3].astype(BF), -1, False)
    from_two = moved((sums[2] + from_three.astype(F32)).astype(BF), -2, True)
    from_one = moved(sums[1].astype(BF), -1, True)
    own = (
        sums[0] + from_one.astype(F32) + from_two.astype(F32) + from_four.astype(F32)
    ).astype(BF)

    both = jnp.concatenate([own, swapped(own, "l")], axis=1)
    first = lax.dynamic_index_in_dim(kv_weight, l, 0, keepdims=False)
    second = lax.dynamic_index_in_dim(kv_weight, 1 - l, 0, keepdims=False)
    input_grad = lax.dot_general(
        both,
        jnp.concatenate([first, second], axis=1),
        (((1,), (1,)), ((), ())),
        preferred_element_type=F32,
    ).astype(BF)

    rows = jnp.concatenate([own] + [turned(own, "y", k) for k in (1, 2, 3)], axis=0)
    norm = 1.0 / math.sqrt(tok * lax.axis_size(SEQ))
    weight_part = lax.dot_general(
        x_rows, rows, (((0,), (0,)), ((), ())), preferred_element_type=F32
    )
    weight_part = (weight_part * norm).reshape(16, 2, width // 32, hd)
    kept = lax.dynamic_index_in_dim(weight_part, c, 1, keepdims=False)
    given = lax.dynamic_index_in_dim(weight_part, 1 - c, 1, keepdims=False)
    total = (kept + swapped(given.astype(BF), "c").astype(F32)).astype(BF)
    spread = lax.all_to_all(total, ("xh", "z"), split_axis=0, concat_axis=0, tiled=True)
    weight_grad = spread.astype(F32).sum(axis=0)
    return (query_grad, input_grad, weight_grad[None])


def solution(mesh):
    finer = Mesh(mesh.devices.reshape(4, 2, 8, 2, 2), ALL)
    placed = (
        P(SEQ, "l"),
        P(SEQ, None),
        P(SEQ, "l"),
        P(SEQ, None),
        P(None, "l", None),
        P(),
    )
    return jax.shard_map(
        local,
        mesh=finer,
        in_specs=placed,
        out_specs=(P(SEQ, "l"), P(SEQ, "l"), P("l", SEQ, None)),
        check_vma=False,
    )
```

```python
import math

import jax
import jax.numpy as jnp
from jax import lax
from jax.experimental import pallas as pl
from jax.experimental.pallas import tpu as pltpu
from jax.sharding import Mesh
from jax.sharding import PartitionSpec as P

WIN = 2048
SEQ = ("y", "xh", "z", "c")
ALL = ("y", "xh", "z", "c", "l")
PAIRS = 64
LINE = 8
BF = jnp.bfloat16
F32 = jnp.float32


def moved(value, steps, flip):
    routes = []
    for source in range(PAIRS):
        target = source + steps
        if not 0 <= target < PAIRS:
            continue
        turn = int(flip and source // LINE != target // LINE)
        for core in range(2):
            for side in range(2):
                routes.append(((source * 2 + core) * 2 + side, (target * 2 + core) * 2 + (side ^ turn)))
    return lax.ppermute(value, ALL, routes)


def swapped(value, axis):
    return lax.ppermute(value, axis, [(0, 1), (1, 0)])


def turned(value, axis, steps):
    count = lax.axis_size(axis)
    return lax.ppermute(value, axis, [(i, (i + steps) % count) for i in range(count)])


def columns(value, which, width):
    return lax.dynamic_slice_in_dim(value, which * width, width, 1)


def attention_kernel(
    side_ref,
    low_ref,
    query_ref,
    out_ref,
    own_ref,
    m1,
    m2,
    m3,
    m4,
    o1,
    o2,
    o3,
    o4,
    near_ref,
    far_ref,
    query_grad_ref,
    given_ref,
    kept_ref,
    keys,
    values,
    queries,
    outs,
    probs,
    dprobs,
    tops,
    turned_grad,
):
    blocks, tok, hd = keys.shape
    heads = query_ref.shape[1] // hd
    inv_root = 1.0 / math.sqrt(hd)
    to_two = inv_root * math.log2(math.e)
    last = blocks - 1
    mine = {1: m1, 2: m2, 3: m3, 4: m4}
    other = {1: o1, 2: o2, 3: o3, 4: o4}
    for h in range(heads):
        queries[h * tok : (h + 1) * tok, :] = query_ref[:, h * hd : (h + 1) * hd]
        outs[h * tok : (h + 1) * tok, :] = out_ref[:, h * hd : (h + 1) * hd]

    @pl.when(side_ref[0] == 0)
    def _():
        for d in mine:
            keys[last - 2 * d] = mine[d][...]
            values[last - 2 * d] = other[d][...]

    @pl.when(side_ref[0] != 0)
    def _():
        for d in mine:
            keys[last - 2 * d] = other[d][...]
            values[last - 2 * d] = mine[d][...]

    keys[last] = own_ref[:, :hd]
    values[last] = own_ref[:, hd:]
    for place, ref, at in ((1, far_ref, 0), (3, far_ref, 1), (5, near_ref, 0), (7, near_ref, 1)):
        keys[place] = ref[at * tok : (at + 1) * tok, :hd]
        values[place] = ref[at * tok : (at + 1) * tok, hd:]

    along = (((1,), (1,)), ((), ()))
    down = (((0,), (0,)), ((), ()))
    low = low_ref[...]
    wide = heads * tok

    def first(block, carry, diagonal):
        top, mass, delta = carry
        row = lax.broadcasted_iota(jnp.int32, (tok, wide), 0)
        ok = row + block * tok >= low
        if diagonal:
            column = lax.broadcasted_iota(jnp.int32, (tok, wide), 1)
            ok = ok & (row <= (column & (tok - 1)))
        scores = lax.dot_general(keys[block], queries[...], along, preferred_element_type=F32)
        dprob = lax.dot_general(values[block], outs[...], along, preferred_element_type=F32)
        scores = jnp.where(ok, scores, -jnp.inf)
        here = jnp.max(scores, axis=0, keepdims=True)
        if not diagonal:
            here = jnp.maximum(here, top)
        prob = jnp.exp2((scores - here) * to_two)
        new_mass = jnp.sum(prob, axis=0, keepdims=True)
        new_delta = jnp.sum(prob * dprob, axis=0, keepdims=True)
        if not diagonal:
            fade = jnp.exp2((top - here) * to_two)
            new_mass = new_mass + mass * fade
            new_delta = new_delta + delta * fade
        probs[block] = prob
        dprobs[block] = dprob
        tops[block] = here
        return here, new_mass, new_delta

    carry = first(last, (None, None, None), True)
    carry = lax.fori_loop(0, last, lambda i, carry: first(i, carry, False), carry)
    top, mass, delta = carry
    inverse = 1.0 / mass
    delta = delta * inverse
    turned_grad[...] = jnp.zeros_like(turned_grad)

    def second(block, ref, at):
        factor = jnp.exp2((tops[block] - top) * to_two) * inverse
        prob = probs[block] * factor
        dscore = (prob * (dprobs[block] - delta)).astype(BF)
        key_grad = jnp.dot(dscore, queries[...], preferred_element_type=F32) * inv_root
        value_grad = jnp.dot(prob.astype(BF), outs[...], preferred_element_type=F32)
        ref[at, :, :hd] = key_grad.astype(BF)
        ref[at, :, hd:] = value_grad.astype(BF)
        turned_grad[...] += lax.dot_general(keys[block], dscore, down, preferred_element_type=F32)

    def odd(i, _):
        second(2 * i + 1, given_ref, i)
        return 0

    def even(i, _):
        second(2 * i, kept_ref, i)
        return 0

    lax.fori_loop(0, blocks // 2, odd, 0)
    lax.fori_loop(0, blocks // 2 + 1, even, 0)
    for h in range(heads):
        part = turned_grad[:, h * tok : (h + 1) * tok] * inv_root
        query_grad_ref[:, h * hd : (h + 1) * hd] = part.T.astype(BF)


def attention(side, low, query, out_grad, own, mine, other, near, far):
    tok, width = query.shape
    hd = own.shape[1] // 2
    heads = width // hd
    wide = heads * tok
    vmem = pl.BlockSpec(memory_space=pltpu.VMEM)
    work = 2 * 5 * wide * 9 * tok * hd
    return pl.pallas_call(
        attention_kernel,
        out_shape=(
            jax.ShapeDtypeStruct((tok, width), BF),
            jax.ShapeDtypeStruct((4, tok, 2 * hd), BF),
            jax.ShapeDtypeStruct((5, tok, 2 * hd), BF),
        ),
        in_specs=[pl.BlockSpec(memory_space=pltpu.SMEM)] + [vmem] * 14,
        out_specs=(vmem, vmem, vmem),
        scratch_shapes=[
            pltpu.VMEM((9, tok, hd), BF),
            pltpu.VMEM((9, tok, hd), BF),
            pltpu.VMEM((wide, hd), BF),
            pltpu.VMEM((wide, hd), BF),
            pltpu.VMEM((9, tok, wide), F32),
            pltpu.VMEM((9, tok, wide), F32),
            pltpu.VMEM((9, 1, wide), F32),
            pltpu.VMEM((hd, wide), F32),
        ],
        compiler_params=pltpu.CompilerParams(vmem_limit_bytes=48 * 1024 * 1024),
        cost_estimate=pl.CostEstimate(
            flops=work, transcendentals=wide * 9 * tok, bytes_accessed=8 * 1024 * 1024
        ),
        name="attention",
    )(side, low, query, out_grad, own, *mine, *other, near, far)


def merge_kernel(one_ref, two_ref, sum_ref):
    sum_ref[...] = (one_ref[...] + two_ref[...].astype(F32)).astype(sum_ref.dtype)


def merged(one, two):
    vmem = pl.BlockSpec(memory_space=pltpu.VMEM)
    return pl.pallas_call(
        merge_kernel,
        out_shape=jax.ShapeDtypeStruct(one.shape, BF),
        in_specs=[vmem, vmem],
        out_specs=vmem,
        compiler_params=pltpu.CompilerParams(vmem_limit_bytes=4 * 1024 * 1024),
        cost_estimate=pl.CostEstimate(flops=one.size, transcendentals=0, bytes_accessed=one.size * 8),
        name="merge",
    )(one, two)


def local(query, key_value, out_grad, inputs_normed, kv_weight, segment_ids):
    tok = query.shape[0]
    hd = key_value.shape[1] // 2
    heads = query.shape[1] // hd
    y, _, z, c, l = (lax.axis_index(axis) for axis in ALL)
    seq_index = lax.axis_index(SEQ)

    def taken(distance):
        turn = (z + distance >= LINE).astype(jnp.int32)
        return columns(key_value, l ^ turn, hd)

    mine, other = {}, {}
    for d in (4, 1, 2, 3):
        mine[d] = moved(taken(d), d, True)
    for d in (1, 2, 3, 4):
        other[d] = swapped(mine[d], "l")
    blocks = {0: key_value}
    for d in (1, 2, 3, 4):
        blocks[d] = jnp.where(
            l == 0,
            jnp.concatenate([mine[d], other[d]], axis=1),
            jnp.concatenate([other[d], mine[d]], axis=1),
        )

    def crossing(low, high):
        return jnp.where(
            c == 0,
            jnp.concatenate([blocks[low + 1], blocks[low]], axis=0),
            jnp.concatenate([blocks[high + 1], blocks[high]], axis=0),
        )

    near = swapped(crossing(0, 1), "c")
    far = swapped(crossing(2, 3), "c")
    width = inputs_normed.shape[1] // 4
    x_parts = [columns(inputs_normed, y, width)]
    for k in (1, 2, 3):
        x_parts.append(turned(columns(inputs_normed, (y + k) % 4, width), "y", k))

    begin = seq_index * tok
    padded = jnp.concatenate([jnp.full((WIN,), -1, jnp.int32), segment_ids], axis=0)
    key_seg = lax.dynamic_slice_in_dim(padded, begin, WIN + tok, 0)
    query_seg = lax.dynamic_slice_in_dim(segment_ids, begin, tok, 0)
    before = jnp.sum((key_seg[:, None] < query_seg[None, :]).astype(jnp.int32), axis=0)
    low = jnp.maximum(before, 1 + jnp.arange(tok, dtype=jnp.int32))
    low = jnp.tile(low, heads)[None, :]
    query_grad, given, kept = attention(
        l.reshape(1).astype(jnp.int32),
        low,
        query,
        out_grad,
        key_value,
        [mine[d] for d in (1, 2, 3, 4)],
        [other[d] for d in (1, 2, 3, 4)],
        near,
        far,
    )
    arrived = swapped(given.reshape(4 * tok, 2 * hd), "c")
    arrived, x_parts = lax.optimization_barrier((arrived, x_parts))
    x_rows = jnp.concatenate(x_parts, axis=0)

    def core_sum(d, which):
        def piece(j):
            if not 0 <= j < 4:
                return jnp.zeros((tok, hd), F32)
            rows = arrived[(3 - j) * tok : (4 - j) * tok]
            return columns(rows, which, hd).astype(F32)

        return columns(kept[4 - d], which, hd).astype(F32) + jnp.where(c == 0, piece(d), piece(d - 1))

    back = {}
    sums = {}
    for d in (4, 3, 2, 1, 0):
        side = l ^ (z < d).astype(jnp.int32)
        got = swapped(core_sum(d, 1 - side).astype(BF), "l")
        sums[d] = (core_sum(d, side), got)
    for d in (3, 4, 2, 1):
        total = merged(*sums[d])
        back[d] = moved(total, -d, True).astype(F32)
    own = (sums[0][0] + sums[0][1].astype(F32) + back[1] + back[2] + back[3] + back[4]).astype(BF)

    partner = swapped(own, "l")
    spread_rows = []
    for k in (1, 2, 3):
        spread_rows.append(turned(own, "y", k))
    partner, spread_rows = lax.optimization_barrier((partner, spread_rows))
    both = jnp.concatenate([own, partner], axis=1)
    first = lax.dynamic_index_in_dim(kv_weight, l, 0, keepdims=False)
    second = lax.dynamic_index_in_dim(kv_weight, 1 - l, 0, keepdims=False)
    input_grad = lax.dot_general(
        both,
        jnp.concatenate([first, second], axis=1),
        (((1,), (1,)), ((), ())),
        preferred_element_type=F32,
    ).astype(BF)

    rows = jnp.concatenate([own] + spread_rows, axis=0)
    norm = 1.0 / math.sqrt(tok * lax.axis_size(SEQ))
    weight_part = lax.dot_general(
        x_rows, rows, (((0,), (0,)), ((), ())), preferred_element_type=F32
    )
    weight_part = (weight_part * norm).reshape(16, 2, width // 32, hd)
    kept = lax.dynamic_index_in_dim(weight_part, c, 1, keepdims=False)
    given = lax.dynamic_index_in_dim(weight_part, 1 - c, 1, keepdims=False)
    total = (kept + swapped(given.astype(BF), "c").astype(F32)).astype(BF)
    spread = lax.all_to_all(total, ("xh", "z"), split_axis=0, concat_axis=0, tiled=True)
    weight_grad = spread.astype(F32).sum(axis=0)
    return (query_grad, input_grad, weight_grad[None])


def solution(mesh):
    finer = Mesh(mesh.devices.reshape(4, 2, 8, 2, 2), ALL)
    placed = (
        P(SEQ, "l"),
        P(SEQ, None),
        P(SEQ, "l"),
        P(SEQ, None),
        P(None, "l", None),
        P(),
    )
    return jax.shard_map(
        local,
        mesh=finer,
        in_specs=placed,
        out_specs=(P(SEQ, "l"), P(SEQ, "l"), P("l", SEQ, None)),
        check_vma=False,
    )
```

```python
import math

import jax
import jax.numpy as jnp
from jax import lax
from jax.experimental import pallas as pl
from jax.experimental.pallas import tpu as pltpu
from jax.sharding import Mesh
from jax.sharding import PartitionSpec as P

WIN = 2048
SEQ = ("y", "xh", "z", "c")
ALL = ("y", "xh", "z", "c", "l")
PAIRS = 64
LINE = 8
BF = jnp.bfloat16
F32 = jnp.float32


def moved(value, steps, flip):
    routes = []
    for source in range(PAIRS):
        target = source + steps
        if not 0 <= target < PAIRS:
            continue
        turn = int(flip and source // LINE != target // LINE)
        for core in range(2):
            for side in range(2):
                routes.append(((source * 2 + core) * 2 + side, (target * 2 + core) * 2 + (side ^ turn)))
    return lax.ppermute(value, ALL, routes)


def swapped(value, axis):
    return lax.ppermute(value, axis, [(0, 1), (1, 0)])


def turned(value, axis, steps):
    count = lax.axis_size(axis)
    return lax.ppermute(value, axis, [(i, (i + steps) % count) for i in range(count)])


def columns(value, which, width):
    return lax.dynamic_slice_in_dim(value, which * width, width, 1)


def attention_kernel(
    side_ref,
    low_ref,
    query_ref,
    out_ref,
    own_ref,
    mine1,
    mine4,
    mine23,
    other1,
    other4,
    other23,
    near_ref,
    far_ref,
    query_grad_ref,
    given_ref,
    kept_ref,
    keys,
    values,
    queries,
    outs,
    probs,
    dprobs,
    tops,
    turned_grad,
):
    blocks, tok, hd = keys.shape
    heads = query_ref.shape[1] // hd
    inv_root = 1.0 / math.sqrt(hd)
    to_two = inv_root * math.log2(math.e)
    last = blocks - 1
    mine = {1: mine1, 4: mine4, 2: mine23.at[:tok], 3: mine23.at[tok:]}
    other = {1: other1, 4: other4, 2: other23.at[:tok], 3: other23.at[tok:]}
    for h in range(heads):
        queries[h * tok : (h + 1) * tok, :] = query_ref[:, h * hd : (h + 1) * hd]
        outs[h * tok : (h + 1) * tok, :] = out_ref[:, h * hd : (h + 1) * hd]

    @pl.when(side_ref[0] == 0)
    def _():
        for d in mine:
            keys[last - 2 * d] = mine[d][...]
            values[last - 2 * d] = other[d][...]

    @pl.when(side_ref[0] != 0)
    def _():
        for d in mine:
            keys[last - 2 * d] = other[d][...]
            values[last - 2 * d] = mine[d][...]

    keys[last] = own_ref[:, :hd]
    values[last] = own_ref[:, hd:]
    for place, ref, at in ((1, far_ref, 0), (3, far_ref, 1), (5, near_ref, 0), (7, near_ref, 1)):
        keys[place] = ref[at * tok : (at + 1) * tok, :hd]
        values[place] = ref[at * tok : (at + 1) * tok, hd:]

    along = (((1,), (1,)), ((), ()))
    down = (((0,), (0,)), ((), ()))
    low = low_ref[...]
    wide = heads * tok

    def first(block, carry, diagonal):
        top, mass, delta = carry
        row = lax.broadcasted_iota(jnp.int32, (tok, wide), 0)
        ok = row + block * tok >= low
        if diagonal:
            column = lax.broadcasted_iota(jnp.int32, (tok, wide), 1)
            ok = ok & (row <= (column & (tok - 1)))
        scores = lax.dot_general(keys[block], queries[...], along, preferred_element_type=F32)
        dprob = lax.dot_general(values[block], outs[...], along, preferred_element_type=F32)
        scores = jnp.where(ok, scores, -jnp.inf)
        here = jnp.max(scores, axis=0, keepdims=True)
        if not diagonal:
            here = jnp.maximum(here, top)
        prob = jnp.exp2((scores - here) * to_two)
        new_mass = jnp.sum(prob, axis=0, keepdims=True)
        new_delta = jnp.sum(prob * dprob, axis=0, keepdims=True)
        if not diagonal:
            fade = jnp.exp2((top - here) * to_two)
            new_mass = new_mass + mass * fade
            new_delta = new_delta + delta * fade
        probs[block] = prob
        dprobs[block] = dprob
        tops[block] = here
        return here, new_mass, new_delta

    carry = first(last, (None, None, None), True)
    carry = lax.fori_loop(0, last, lambda i, carry: first(i, carry, False), carry)
    top, mass, delta = carry
    inverse = 1.0 / mass
    delta = delta * inverse
    turned_grad[...] = jnp.zeros_like(turned_grad)

    def second(block, ref, at):
        factor = jnp.exp2((tops[block] - top) * to_two) * inverse
        prob = probs[block] * factor
        dscore = (prob * (dprobs[block] - delta)).astype(BF)
        key_grad = jnp.dot(dscore, queries[...], preferred_element_type=F32) * inv_root
        value_grad = jnp.dot(prob.astype(BF), outs[...], preferred_element_type=F32)
        ref[at, :, :hd] = key_grad.astype(BF)
        ref[at, :, hd:] = value_grad.astype(BF)
        turned_grad[...] += lax.dot_general(keys[block], dscore, down, preferred_element_type=F32)

    def odd(i, _):
        second(2 * i + 1, given_ref, i)
        return 0

    def even(i, _):
        second(2 * i, kept_ref, i)
        return 0

    lax.fori_loop(0, blocks // 2, odd, 0)
    lax.fori_loop(0, blocks // 2 + 1, even, 0)
    for h in range(heads):
        part = turned_grad[:, h * tok : (h + 1) * tok] * inv_root
        query_grad_ref[:, h * hd : (h + 1) * hd] = part.T.astype(BF)


def attention(side, low, query, out_grad, own, mine, other, near, far):
    tok, width = query.shape
    hd = own.shape[1] // 2
    heads = width // hd
    wide = heads * tok
    vmem = pl.BlockSpec(memory_space=pltpu.VMEM)
    work = 2 * 5 * wide * 9 * tok * hd
    return pl.pallas_call(
        attention_kernel,
        out_shape=(
            jax.ShapeDtypeStruct((tok, width), BF),
            jax.ShapeDtypeStruct((4, tok, 2 * hd), BF),
            jax.ShapeDtypeStruct((5, tok, 2 * hd), BF),
        ),
        in_specs=[pl.BlockSpec(memory_space=pltpu.SMEM)] + [vmem] * 12,
        out_specs=(vmem, vmem, vmem),
        scratch_shapes=[
            pltpu.VMEM((9, tok, hd), BF),
            pltpu.VMEM((9, tok, hd), BF),
            pltpu.VMEM((wide, hd), BF),
            pltpu.VMEM((wide, hd), BF),
            pltpu.VMEM((9, tok, wide), F32),
            pltpu.VMEM((9, tok, wide), F32),
            pltpu.VMEM((9, 1, wide), F32),
            pltpu.VMEM((hd, wide), F32),
        ],
        compiler_params=pltpu.CompilerParams(vmem_limit_bytes=48 * 1024 * 1024),
        cost_estimate=pl.CostEstimate(
            flops=work, transcendentals=wide * 9 * tok, bytes_accessed=8 * 1024 * 1024
        ),
        name="attention",
    )(side, low, query, out_grad, own, *mine, *other, near, far)


def merge_kernel(*refs):
    parts, sum_ref = refs[:-1], refs[-1]
    total = parts[0][...].astype(F32)
    for part in parts[1:]:
        total = total + part[...].astype(F32)
    sum_ref[...] = total.astype(sum_ref.dtype)


def merged(*parts):
    vmem = pl.BlockSpec(memory_space=pltpu.VMEM)
    size = parts[0].size
    return pl.pallas_call(
        merge_kernel,
        out_shape=jax.ShapeDtypeStruct(parts[0].shape, BF),
        in_specs=[vmem] * len(parts),
        out_specs=vmem,
        compiler_params=pltpu.CompilerParams(vmem_limit_bytes=4 * 1024 * 1024),
        cost_estimate=pl.CostEstimate(flops=size, transcendentals=0, bytes_accessed=size * 8),
        name="merge",
    )(*parts)


def local(query, key_value, out_grad, inputs_normed, kv_weight, segment_ids):
    tok = query.shape[0]
    hd = key_value.shape[1] // 2
    heads = query.shape[1] // hd
    y, _, z, c, l = (lax.axis_index(axis) for axis in ALL)
    seq_index = lax.axis_index(SEQ)

    def taken(distance):
        turn = (z + distance >= LINE).astype(jnp.int32)
        return columns(key_value, l ^ turn, hd)

    mine1 = moved(taken(1), 1, True)
    mine4 = moved(taken(4), 4, True)
    mine23 = moved(jnp.concatenate([columns(key_value, l, hd), mine1], axis=0), 2, False)
    other1 = swapped(mine1, "l")
    other4 = swapped(mine4, "l")
    other23 = swapped(mine23, "l")
    mine = {1: mine1, 4: mine4, 2: mine23[:tok], 3: mine23[tok:]}
    other = {1: other1, 4: other4, 2: other23[:tok], 3: other23[tok:]}
    blocks = {0: key_value}
    for d in (1, 2, 3, 4):
        blocks[d] = jnp.where(
            l == 0,
            jnp.concatenate([mine[d], other[d]], axis=1),
            jnp.concatenate([other[d], mine[d]], axis=1),
        )

    def crossing(low, high):
        return jnp.where(
            c == 0,
            jnp.concatenate([blocks[low + 1], blocks[low]], axis=0),
            jnp.concatenate([blocks[high + 1], blocks[high]], axis=0),
        )

    near = swapped(crossing(0, 1), "c")
    far = swapped(crossing(2, 3), "c")
    width = inputs_normed.shape[1] // 4
    x_parts = [columns(inputs_normed, y, width)]
    for k in (1, 2, 3):
        x_parts.append(turned(columns(inputs_normed, (y + k) % 4, width), "y", k))

    begin = seq_index * tok
    padded = jnp.concatenate([jnp.full((WIN,), -1, jnp.int32), segment_ids], axis=0)
    key_seg = lax.dynamic_slice_in_dim(padded, begin, WIN + tok, 0)
    query_seg = lax.dynamic_slice_in_dim(segment_ids, begin, tok, 0)
    before = jnp.sum((key_seg[:, None] < query_seg[None, :]).astype(jnp.int32), axis=0)
    low = jnp.maximum(before, 1 + jnp.arange(tok, dtype=jnp.int32))
    low = jnp.tile(low, heads)[None, :]
    query_grad, given, kept = attention(
        l.reshape(1).astype(jnp.int32),
        low,
        query,
        out_grad,
        key_value,
        (mine1, mine4, mine23),
        (other1, other4, other23),
        near,
        far,
    )
    arrived = swapped(given.reshape(4 * tok, 2 * hd), "c")
    arrived, x_parts = lax.optimization_barrier((arrived, x_parts))
    x_rows = jnp.concatenate(x_parts, axis=0)

    def core_sum(d, which):
        def piece(j):
            if not 0 <= j < 4:
                return jnp.zeros((tok, hd), F32)
            rows = arrived[(3 - j) * tok : (4 - j) * tok]
            return columns(rows, which, hd).astype(F32)

        return columns(kept[4 - d], which, hd).astype(F32) + jnp.where(c == 0, piece(d), piece(d - 1))

    sides = {
        4: l ^ (z < 4).astype(jnp.int32),
        3: l ^ ((z + LINE - 2) % LINE < 1).astype(jnp.int32),
        2: l,
        1: l ^ (z < 1).astype(jnp.int32),
        0: l,
    }

    def paired(*distances):
        keep = jnp.concatenate([core_sum(d, sides[d]) for d in distances], axis=0)
        give = jnp.concatenate([core_sum(d, 1 - sides[d]).astype(BF) for d in distances], axis=0)
        return keep, swapped(give, "l")

    two_three = merged(*paired(2, 3))
    four = merged(*paired(4))
    one = paired(1)
    none = paired(0)
    back23 = moved(two_three, -2, False)
    back4 = moved(four, -4, True)
    one = merged(*one, back23[tok:])
    back1 = moved(one, -1, True)
    own = sum(part.astype(F32) for part in (*none, back23[:tok], back1, back4)).astype(BF)

    partner = swapped(own, "l")
    spread_rows = []
    for k in (1, 2, 3):
        spread_rows.append(turned(own, "y", k))
    partner, spread_rows = lax.optimization_barrier((partner, spread_rows))
    both = jnp.concatenate([own, partner], axis=1)
    first = lax.dynamic_index_in_dim(kv_weight, l, 0, keepdims=False)
    second = lax.dynamic_index_in_dim(kv_weight, 1 - l, 0, keepdims=False)
    input_grad = lax.dot_general(
        both,
        jnp.concatenate([first, second], axis=1),
        (((1,), (1,)), ((), ())),
        preferred_element_type=F32,
    ).astype(BF)

    rows = jnp.concatenate([own] + spread_rows, axis=0)
    norm = 1.0 / math.sqrt(tok * lax.axis_size(SEQ))
    weight_part = lax.dot_general(
        x_rows, rows, (((0,), (0,)), ((), ())), preferred_element_type=F32
    )
    weight_part = (weight_part * norm).reshape(16, 2, width // 32, hd)
    kept = lax.dynamic_index_in_dim(weight_part, c, 1, keepdims=False)
    given = lax.dynamic_index_in_dim(weight_part, 1 - c, 1, keepdims=False)
    total = (kept + swapped(given.astype(BF), "c").astype(F32)).astype(BF)
    spread = lax.all_to_all(total, ("xh", "z"), split_axis=0, concat_axis=0, tiled=True)
    weight_grad = spread.astype(F32).sum(axis=0)
    return (query_grad, input_grad, weight_grad[None])


def solution(mesh):
    finer = Mesh(mesh.devices.reshape(4, 2, 8, 2, 2), ALL)
    placed = (
        P(SEQ, "l"),
        P(SEQ, None),
        P(SEQ, "l"),
        P(SEQ, None),
        P(None, "l", None),
        P(),
    )
    return jax.shard_map(
        local,
        mesh=finer,
        in_specs=placed,
        out_specs=(P(SEQ, "l"), P(SEQ, "l"), P("l", SEQ, None)),
        check_vma=False,
    )
```

```python
import math

import jax
import jax.numpy as jnp
from jax import lax
from jax.experimental import pallas as pl
from jax.experimental.pallas import tpu as pltpu
from jax.sharding import Mesh
from jax.sharding import PartitionSpec as P

WIN = 2048
SEQ = ("y", "xh", "z", "c")
ALL = ("y", "xh", "z", "c", "l")
PAIRS = 64
LINE = 8
BF = jnp.bfloat16
F32 = jnp.float32


def moved(value, steps, flip):
    routes = []
    for source in range(PAIRS):
        target = source + steps
        if not 0 <= target < PAIRS:
            continue
        turn = int(flip and source // LINE != target // LINE)
        for core in range(2):
            for side in range(2):
                routes.append(((source * 2 + core) * 2 + side, (target * 2 + core) * 2 + (side ^ turn)))
    return lax.ppermute(value, ALL, routes)


def swapped(value, axis):
    return lax.ppermute(value, axis, [(0, 1), (1, 0)])


def turned(value, axis, steps):
    count = lax.axis_size(axis)
    return lax.ppermute(value, axis, [(i, (i + steps) % count) for i in range(count)])


def columns(value, which, width):
    return lax.dynamic_slice_in_dim(value, which * width, width, 1)


def attention_kernel(
    side_ref,
    low_ref,
    query_ref,
    out_ref,
    own_ref,
    mine1,
    mine4,
    mine23,
    other1,
    other4,
    other23,
    near_ref,
    far_ref,
    query_grad_ref,
    given_ref,
    kept_ref,
    keys,
    values,
    queries,
    outs,
    probs,
    dprobs,
    tops,
    turned_grad,
):
    blocks, tok, hd = keys.shape
    heads = query_ref.shape[1] // hd
    inv_root = 1.0 / math.sqrt(hd)
    to_two = inv_root * math.log2(math.e)
    last = blocks - 1
    mine = {1: mine1, 4: mine4, 2: mine23.at[:tok], 3: mine23.at[tok:]}
    other = {1: other1, 4: other4, 2: other23.at[:tok], 3: other23.at[tok:]}
    for h in range(heads):
        queries[h * tok : (h + 1) * tok, :] = query_ref[:, h * hd : (h + 1) * hd]
        outs[h * tok : (h + 1) * tok, :] = out_ref[:, h * hd : (h + 1) * hd]

    for d in mine:
        side = side_ref[1 if d == 1 else 0]

        @pl.when(side == 0)
        def _():
            keys[last - 2 * d] = mine[d][...]
            values[last - 2 * d] = other[d][...]

        @pl.when(side != 0)
        def _():
            keys[last - 2 * d] = other[d][...]
            values[last - 2 * d] = mine[d][...]

    keys[last] = own_ref[:, :hd]
    values[last] = own_ref[:, hd:]
    for place, ref, at in ((1, far_ref, 0), (3, far_ref, 1), (5, near_ref, 0), (7, near_ref, 1)):
        keys[place] = ref[at * tok : (at + 1) * tok, :hd]
        values[place] = ref[at * tok : (at + 1) * tok, hd:]

    along = (((1,), (1,)), ((), ()))
    down = (((0,), (0,)), ((), ()))
    low = low_ref[...]
    wide = heads * tok

    def first(block, carry, diagonal):
        top, mass, delta = carry
        row = lax.broadcasted_iota(jnp.int32, (tok, wide), 0)
        ok = row + block * tok >= low
        if diagonal:
            column = lax.broadcasted_iota(jnp.int32, (tok, wide), 1)
            ok = ok & (row <= (column & (tok - 1)))
        scores = lax.dot_general(keys[block], queries[...], along, preferred_element_type=F32)
        dprob = lax.dot_general(values[block], outs[...], along, preferred_element_type=F32)
        scores = jnp.where(ok, scores, -jnp.inf)
        here = jnp.max(scores, axis=0, keepdims=True)
        if not diagonal:
            here = jnp.maximum(here, top)
        prob = jnp.exp2((scores - here) * to_two)
        new_mass = jnp.sum(prob, axis=0, keepdims=True)
        new_delta = jnp.sum(prob * dprob, axis=0, keepdims=True)
        if not diagonal:
            fade = jnp.exp2((top - here) * to_two)
            new_mass = new_mass + mass * fade
            new_delta = new_delta + delta * fade
        probs[block] = prob
        dprobs[block] = dprob
        tops[block] = here
        return here, new_mass, new_delta

    carry = first(last, (None, None, None), True)
    carry = lax.fori_loop(0, last, lambda i, carry: first(i, carry, False), carry)
    top, mass, delta = carry
    inverse = 1.0 / mass
    delta = delta * inverse
    turned_grad[...] = jnp.zeros_like(turned_grad)

    def second(block, ref, at):
        factor = jnp.exp2((tops[block] - top) * to_two) * inverse
        prob = probs[block] * factor
        dscore = (prob * (dprobs[block] - delta)).astype(BF)
        key_grad = jnp.dot(dscore, queries[...], preferred_element_type=F32) * inv_root
        value_grad = jnp.dot(prob.astype(BF), outs[...], preferred_element_type=F32)
        ref[at, :, :hd] = key_grad.astype(BF)
        ref[at, :, hd:] = value_grad.astype(BF)
        turned_grad[...] += lax.dot_general(keys[block], dscore, down, preferred_element_type=F32)

    def odd(i, _):
        second(2 * i + 1, given_ref, i)
        return 0

    def even(i, _):
        second(2 * i, kept_ref, i)
        return 0

    lax.fori_loop(0, blocks // 2, odd, 0)
    lax.fori_loop(0, blocks // 2 + 1, even, 0)
    for h in range(heads):
        part = turned_grad[:, h * tok : (h + 1) * tok] * inv_root
        query_grad_ref[:, h * hd : (h + 1) * hd] = part.T.astype(BF)


def attention(side, low, query, out_grad, own, mine, other, near, far):
    tok, width = query.shape
    hd = own.shape[1] // 2
    heads = width // hd
    wide = heads * tok
    vmem = pl.BlockSpec(memory_space=pltpu.VMEM)
    work = 2 * 5 * wide * 9 * tok * hd
    return pl.pallas_call(
        attention_kernel,
        out_shape=(
            jax.ShapeDtypeStruct((tok, width), BF),
            jax.ShapeDtypeStruct((4, tok, 2 * hd), BF),
            jax.ShapeDtypeStruct((5, tok, 2 * hd), BF),
        ),
        in_specs=[pl.BlockSpec(memory_space=pltpu.SMEM)] + [vmem] * 12,
        out_specs=(vmem, vmem, vmem),
        scratch_shapes=[
            pltpu.VMEM((9, tok, hd), BF),
            pltpu.VMEM((9, tok, hd), BF),
            pltpu.VMEM((wide, hd), BF),
            pltpu.VMEM((wide, hd), BF),
            pltpu.VMEM((9, tok, wide), F32),
            pltpu.VMEM((9, tok, wide), F32),
            pltpu.VMEM((9, 1, wide), F32),
            pltpu.VMEM((hd, wide), F32),
        ],
        compiler_params=pltpu.CompilerParams(vmem_limit_bytes=48 * 1024 * 1024),
        cost_estimate=pl.CostEstimate(
            flops=work, transcendentals=wide * 9 * tok, bytes_accessed=8 * 1024 * 1024
        ),
        name="attention",
    )(side, low, query, out_grad, own, *mine, *other, near, far)


def merge_kernel(*refs):
    parts, sum_ref = refs[:-1], refs[-1]
    total = parts[0][...].astype(F32)
    for part in parts[1:]:
        total = total + part[...].astype(F32)
    sum_ref[...] = total.astype(sum_ref.dtype)


def merged(*parts):
    vmem = pl.BlockSpec(memory_space=pltpu.VMEM)
    size = parts[0].size
    return pl.pallas_call(
        merge_kernel,
        out_shape=jax.ShapeDtypeStruct(parts[0].shape, BF),
        in_specs=[vmem] * len(parts),
        out_specs=vmem,
        compiler_params=pltpu.CompilerParams(vmem_limit_bytes=4 * 1024 * 1024),
        cost_estimate=pl.CostEstimate(flops=size, transcendentals=0, bytes_accessed=size * 8),
        name="merge",
    )(*parts)


def local(query, key_value, out_grad, inputs_normed, kv_weight, segment_ids):
    tok = query.shape[0]
    hd = key_value.shape[1] // 2
    heads = query.shape[1] // hd
    y, _, z, c, l = (lax.axis_index(axis) for axis in ALL)
    seq_index = lax.axis_index(SEQ)

    def taken(distance):
        turn = (z + distance >= LINE).astype(jnp.int32)
        return columns(key_value, l ^ turn, hd)

    ahead = (z >= LINE - 2).astype(jnp.int32)
    ahead_next = ((z + 1) % LINE >= LINE - 2).astype(jnp.int32)
    turn = (z + 1 >= LINE).astype(jnp.int32)
    mine1 = moved(columns(key_value, l ^ turn ^ ahead_next, hd), 1, True)
    mine4 = moved(taken(4), 4, True)
    mine23 = moved(jnp.concatenate([taken(2), mine1], axis=0), 2, True)
    other1 = swapped(mine1, "l")
    other4 = swapped(mine4, "l")
    other23 = swapped(mine23, "l")
    mine = {1: mine1, 4: mine4, 2: mine23[:tok], 3: mine23[tok:]}
    other = {1: other1, 4: other4, 2: other23[:tok], 3: other23[tok:]}
    blocks = {0: key_value}
    for d in (1, 2, 3, 4):
        blocks[d] = jnp.where(
            (l ^ ahead if d == 1 else l) == 0,
            jnp.concatenate([mine[d], other[d]], axis=1),
            jnp.concatenate([other[d], mine[d]], axis=1),
        )

    def crossing(low, high):
        return jnp.where(
            c == 0,
            jnp.concatenate([blocks[low + 1], blocks[low]], axis=0),
            jnp.concatenate([blocks[high + 1], blocks[high]], axis=0),
        )

    near = swapped(crossing(0, 1), "c")
    far = swapped(crossing(2, 3), "c")
    width = inputs_normed.shape[1] // 4
    x_parts = [columns(inputs_normed, y, width)]
    for k in (1, 2, 3):
        x_parts.append(turned(columns(inputs_normed, (y + k) % 4, width), "y", k))

    begin = seq_index * tok
    padded = jnp.concatenate([jnp.full((WIN,), -1, jnp.int32), segment_ids], axis=0)
    key_seg = lax.dynamic_slice_in_dim(padded, begin, WIN + tok, 0)
    query_seg = lax.dynamic_slice_in_dim(segment_ids, begin, tok, 0)
    before = jnp.sum((key_seg[:, None] < query_seg[None, :]).astype(jnp.int32), axis=0)
    low = jnp.maximum(before, 1 + jnp.arange(tok, dtype=jnp.int32))
    low = jnp.tile(low, heads)[None, :]
    query_grad, given, kept = attention(
        jnp.stack([l, l ^ ahead]).astype(jnp.int32),
        low,
        query,
        out_grad,
        key_value,
        (mine1, mine4, mine23),
        (other1, other4, other23),
        near,
        far,
    )
    arrived = swapped(given.reshape(4 * tok, 2 * hd), "c")
    arrived, x_parts = lax.optimization_barrier((arrived, x_parts))
    x_rows = jnp.concatenate(x_parts, axis=0)

    def core_sum(d, which):
        def piece(j):
            if not 0 <= j < 4:
                return jnp.zeros((tok, hd), F32)
            rows = arrived[(3 - j) * tok : (4 - j) * tok]
            return columns(rows, which, hd).astype(F32)

        return columns(kept[4 - d], which, hd).astype(F32) + jnp.where(c == 0, piece(d), piece(d - 1))

    sides = {
        4: l ^ (z < 4).astype(jnp.int32),
        3: l ^ (z < 3).astype(jnp.int32),
        2: l ^ (z < 2).astype(jnp.int32),
        1: l ^ (z < 1).astype(jnp.int32),
        0: l,
    }

    def paired(*distances):
        keep = jnp.concatenate([core_sum(d, sides[d]) for d in distances], axis=0)
        give = jnp.concatenate([core_sum(d, 1 - sides[d]).astype(BF) for d in distances], axis=0)
        return keep, swapped(give, "l")

    two_three = merged(*paired(2, 3))
    four = merged(*paired(4))
    one = paired(1)
    none = paired(0)
    back23 = moved(two_three, -2, True)
    back4 = moved(four, -4, True)
    one = merged(*one, back23[tok:])
    back1 = moved(one, -1, True)
    own = sum(part.astype(F32) for part in (*none, back23[:tok], back1, back4)).astype(BF)

    partner = swapped(own, "l")
    spread_rows = []
    for k in (1, 2, 3):
        spread_rows.append(turned(own, "y", k))
    partner, spread_rows = lax.optimization_barrier((partner, spread_rows))
    both = jnp.concatenate([own, partner], axis=1)
    first = lax.dynamic_index_in_dim(kv_weight, l, 0, keepdims=False)
    second = lax.dynamic_index_in_dim(kv_weight, 1 - l, 0, keepdims=False)
    input_grad = lax.dot_general(
        both,
        jnp.concatenate([first, second], axis=1),
        (((1,), (1,)), ((), ())),
        preferred_element_type=F32,
    ).astype(BF)

    rows = jnp.concatenate([own] + spread_rows, axis=0)
    norm = 1.0 / math.sqrt(tok * lax.axis_size(SEQ))
    weight_part = lax.dot_general(
        x_rows, rows, (((0,), (0,)), ((), ())), preferred_element_type=F32
    )
    weight_part = (weight_part * norm).reshape(16, 2, width // 32, hd)
    kept = lax.dynamic_index_in_dim(weight_part, c, 1, keepdims=False)
    given = lax.dynamic_index_in_dim(weight_part, 1 - c, 1, keepdims=False)
    total = (kept + swapped(given.astype(BF), "c").astype(F32)).astype(BF)
    spread = lax.all_to_all(total, ("xh", "z"), split_axis=0, concat_axis=0, tiled=True)
    weight_grad = spread.astype(F32).sum(axis=0)
    return (query_grad, input_grad, weight_grad[None])


def solution(mesh):
    finer = Mesh(mesh.devices.reshape(4, 2, 8, 2, 2), ALL)
    placed = (
        P(SEQ, "l"),
        P(SEQ, None),
        P(SEQ, "l"),
        P(SEQ, None),
        P(None, "l", None),
        P(),
    )
    return jax.shard_map(
        local,
        mesh=finer,
        in_specs=placed,
        out_specs=(P(SEQ, "l"), P(SEQ, "l"), P("l", SEQ, None)),
        check_vma=False,
    )
```

```python
import math

import jax
import jax.numpy as jnp
from jax import lax
from jax.experimental import pallas as pl
from jax.experimental.pallas import tpu as pltpu
from jax.sharding import Mesh
from jax.sharding import PartitionSpec as P

WIN = 2048
SEQ = ("y", "xh", "z", "c")
ALL = ("y", "xh", "z", "c", "l")
PAIRS = 64
LINE = 8
BF = jnp.bfloat16
F32 = jnp.float32


def moved(value, steps, flip):
    routes = []
    for source in range(PAIRS):
        target = source + steps
        if not 0 <= target < PAIRS:
            continue
        turn = int(flip and source // LINE != target // LINE)
        for core in range(2):
            for side in range(2):
                routes.append(((source * 2 + core) * 2 + side, (target * 2 + core) * 2 + (side ^ turn)))
    return lax.ppermute(value, ALL, routes)


def swapped(value, axis):
    return lax.ppermute(value, axis, [(0, 1), (1, 0)])


def turned(value, axis, steps):
    count = lax.axis_size(axis)
    return lax.ppermute(value, axis, [(i, (i + steps) % count) for i in range(count)])


def columns(value, which, width):
    return lax.dynamic_slice_in_dim(value, which * width, width, 1)


def attention_kernel(
    side_ref,
    low_ref,
    query_ref,
    out_ref,
    own_ref,
    m1,
    m2,
    m3,
    m4,
    o1,
    o2,
    o3,
    o4,
    near_ref,
    far_ref,
    query_grad_ref,
    given_ref,
    kept_ref,
    keys,
    values,
    queries,
    outs,
    probs,
    dprobs,
    tops,
    turned_grad,
):
    blocks, tok, hd = keys.shape
    heads = query_ref.shape[1] // hd
    inv_root = 1.0 / math.sqrt(hd)
    to_two = inv_root * math.log2(math.e)
    last = blocks - 1
    mine = {1: m1, 2: m2, 3: m3, 4: m4}
    other = {1: o1, 2: o2, 3: o3, 4: o4}
    for h in range(heads):
        queries[h * tok : (h + 1) * tok, :] = query_ref[:, h * hd : (h + 1) * hd]
        outs[h * tok : (h + 1) * tok, :] = out_ref[:, h * hd : (h + 1) * hd]

    @pl.when(side_ref[0] == 0)
    def _():
        for d in mine:
            keys[last - 2 * d] = mine[d][...]
            values[last - 2 * d] = other[d][...]

    @pl.when(side_ref[0] != 0)
    def _():
        for d in mine:
            keys[last - 2 * d] = other[d][...]
            values[last - 2 * d] = mine[d][...]

    keys[last] = own_ref[:, :hd]
    values[last] = own_ref[:, hd:]
    for place, ref, at in ((1, far_ref, 0), (3, far_ref, 1), (5, near_ref, 0), (7, near_ref, 1)):
        keys[place] = ref[at * tok : (at + 1) * tok, :hd]
        values[place] = ref[at * tok : (at + 1) * tok, hd:]

    along = (((1,), (1,)), ((), ()))
    down = (((0,), (0,)), ((), ()))
    low = low_ref[...]
    wide = heads * tok

    def first(block, carry, diagonal):
        top, mass, delta = carry
        row = lax.broadcasted_iota(jnp.int32, (tok, wide), 0)
        ok = row >= low - block * tok
        if diagonal:
            column = lax.broadcasted_iota(jnp.int32, (tok, wide), 1)
            ok = ok & (row <= (column & (tok - 1)))
        scores = lax.dot_general(keys[block], queries[...], along, preferred_element_type=F32)
        dprob = lax.dot_general(values[block], outs[...], along, preferred_element_type=F32)
        scores = jnp.where(ok, scores, -jnp.inf)
        here = jnp.max(scores, axis=0, keepdims=True)
        if not diagonal:
            here = jnp.maximum(here, top)
        prob = jnp.exp2((scores - here) * to_two)
        new_mass = jnp.sum(prob, axis=0, keepdims=True)
        new_delta = jnp.sum(prob * dprob, axis=0, keepdims=True)
        if not diagonal:
            fade = jnp.exp2((top - here) * to_two)
            new_mass = new_mass + mass * fade
            new_delta = new_delta + delta * fade
        probs[block] = prob
        dprobs[block] = dprob
        tops[block] = here
        return here, new_mass, new_delta

    carry = first(last, (None, None, None), True)
    carry = lax.fori_loop(0, last, lambda i, carry: first(i, carry, False), carry)
    top, mass, delta = carry
    inverse = 1.0 / mass
    delta = delta * inverse
    turned_grad[...] = jnp.zeros_like(turned_grad)

    def second(block, ref, at):
        factor = jnp.exp2((tops[block] - top) * to_two) * inverse
        prob = probs[block] * factor
        dscore = (prob * (dprobs[block] - delta)).astype(BF)
        key_grad = jnp.dot(dscore, queries[...], preferred_element_type=F32) * inv_root
        value_grad = jnp.dot(prob.astype(BF), outs[...], preferred_element_type=F32)
        ref[at, :, :hd] = key_grad.astype(BF)
        ref[at, :, hd:] = value_grad.astype(BF)
        turned_grad[...] += lax.dot_general(keys[block], dscore, down, preferred_element_type=F32)

    def odd(i, _):
        second(2 * i + 1, given_ref, i)
        return 0

    def even(i, _):
        second(2 * i, kept_ref, i)
        return 0

    lax.fori_loop(0, blocks // 2, odd, 0)
    lax.fori_loop(0, blocks // 2 + 1, even, 0)
    for h in range(heads):
        part = turned_grad[:, h * tok : (h + 1) * tok] * inv_root
        query_grad_ref[:, h * hd : (h + 1) * hd] = part.T.astype(BF)


def attention(side, low, query, out_grad, own, mine, other, near, far):
    tok, width = query.shape
    hd = own.shape[1] // 2
    heads = width // hd
    wide = heads * tok
    vmem = pl.BlockSpec(memory_space=pltpu.VMEM)
    work = 2 * 5 * wide * 9 * tok * hd
    return pl.pallas_call(
        attention_kernel,
        out_shape=(
            jax.ShapeDtypeStruct((tok, width), BF),
            jax.ShapeDtypeStruct((4, tok, 2 * hd), BF),
            jax.ShapeDtypeStruct((5, tok, 2 * hd), BF),
        ),
        in_specs=[pl.BlockSpec(memory_space=pltpu.SMEM)] + [vmem] * 14,
        out_specs=(vmem, vmem, vmem),
        scratch_shapes=[
            pltpu.VMEM((9, tok, hd), BF),
            pltpu.VMEM((9, tok, hd), BF),
            pltpu.VMEM((wide, hd), BF),
            pltpu.VMEM((wide, hd), BF),
            pltpu.VMEM((9, tok, wide), F32),
            pltpu.VMEM((9, tok, wide), F32),
            pltpu.VMEM((9, 1, wide), F32),
            pltpu.VMEM((hd, wide), F32),
        ],
        compiler_params=pltpu.CompilerParams(vmem_limit_bytes=48 * 1024 * 1024),
        cost_estimate=pl.CostEstimate(
            flops=work, transcendentals=wide * 9 * tok, bytes_accessed=8 * 1024 * 1024
        ),
        name="attention",
    )(side, low, query, out_grad, own, *mine, *other, near, far)


def merge_kernel(one_ref, two_ref, sum_ref):
    sum_ref[...] = (one_ref[...] + two_ref[...].astype(F32)).astype(sum_ref.dtype)


def merged(one, two):
    vmem = pl.BlockSpec(memory_space=pltpu.VMEM)
    return pl.pallas_call(
        merge_kernel,
        out_shape=jax.ShapeDtypeStruct(one.shape, BF),
        in_specs=[vmem, vmem],
        out_specs=vmem,
        compiler_params=pltpu.CompilerParams(vmem_limit_bytes=4 * 1024 * 1024),
        cost_estimate=pl.CostEstimate(flops=one.size, transcendentals=0, bytes_accessed=one.size * 8),
        name="merge",
    )(one, two)


def core_merge_kernel(core_ref, own_ref, arrived_ref, sum_ref):
    total = own_ref[:, core_ref[0]] + arrived_ref[...].astype(F32)
    sum_ref[...] = total.astype(BF)


def core_merged(core, own, arrived):
    vmem = pl.BlockSpec(memory_space=pltpu.VMEM)
    size = arrived.size
    return pl.pallas_call(
        core_merge_kernel,
        out_shape=jax.ShapeDtypeStruct(arrived.shape, BF),
        in_specs=[pl.BlockSpec(memory_space=pltpu.SMEM), vmem, vmem],
        out_specs=vmem,
        compiler_params=pltpu.CompilerParams(vmem_limit_bytes=8 * 1024 * 1024),
        cost_estimate=pl.CostEstimate(flops=size, transcendentals=0, bytes_accessed=size * 8),
        name="core_merge",
    )(core.reshape(1).astype(jnp.int32), own, arrived)


def local(query, key_value, out_grad, inputs_normed, kv_weight, segment_ids):
    tok = query.shape[0]
    hd = key_value.shape[1] // 2
    heads = query.shape[1] // hd
    y, _, z, c, l = (lax.axis_index(axis) for axis in ALL)
    seq_index = lax.axis_index(SEQ)

    def taken(distance):
        turn = (z + distance >= LINE).astype(jnp.int32)
        return columns(key_value, l ^ turn, hd)

    mine, other = {}, {}
    for d in (3, 4, 2, 1):
        mine[d] = moved(taken(d), d, True)
    for d in (1, 2, 3, 4):
        other[d] = swapped(mine[d], "l")
    blocks = {0: key_value}
    for d in (1, 2, 3, 4):
        blocks[d] = jnp.where(
            l == 0,
            jnp.concatenate([mine[d], other[d]], axis=1),
            jnp.concatenate([other[d], mine[d]], axis=1),
        )

    def crossing(low, high):
        return jnp.where(
            c == 0,
            jnp.concatenate([blocks[low + 1], blocks[low]], axis=0),
            jnp.concatenate([blocks[high + 1], blocks[high]], axis=0),
        )

    near = swapped(crossing(0, 1), "c")
    far = swapped(crossing(2, 3), "c")
    width = inputs_normed.shape[1] // 4
    x_parts = [columns(inputs_normed, y, width)]
    for k in (1, 2, 3):
        x_parts.append(turned(columns(inputs_normed, (y + k) % 4, width), "y", k))

    begin = seq_index * tok
    padded = jnp.concatenate([jnp.full((WIN,), -1, jnp.int32), segment_ids], axis=0)
    key_seg = lax.dynamic_slice_in_dim(padded, begin, WIN + tok, 0)
    query_seg = lax.dynamic_slice_in_dim(segment_ids, begin, tok, 0)
    before = jnp.sum((key_seg[:, None] < query_seg[None, :]).astype(jnp.int32), axis=0)
    low = jnp.maximum(before, 1 + jnp.arange(tok, dtype=jnp.int32))
    low = jnp.tile(low, heads)[None, :]
    query_grad, given, kept = attention(
        l.reshape(1).astype(jnp.int32),
        low,
        query,
        out_grad,
        key_value,
        [mine[d] for d in (1, 2, 3, 4)],
        [other[d] for d in (1, 2, 3, 4)],
        near,
        far,
    )
    arrived = swapped(given.reshape(4 * tok, 2 * hd), "c")
    x_rows = jnp.concatenate(x_parts, axis=0)

    def core_sum(d, which):
        def piece(j):
            if not 0 <= j < 4:
                return jnp.zeros((tok, hd), F32)
            rows = arrived[(3 - j) * tok : (4 - j) * tok]
            return columns(rows, which, hd).astype(F32)

        return columns(kept[4 - d], which, hd).astype(F32) + jnp.where(c == 0, piece(d), piece(d - 1))

    back = {}
    sums = {}
    for d in (4, 3, 2, 1, 0):
        side = l ^ (z < d).astype(jnp.int32)
        got = swapped(core_sum(d, 1 - side).astype(BF), "l")
        sums[d] = (core_sum(d, side), got)
    for d in (3, 4, 2, 1):
        total = merged(*sums[d])
        back[d] = moved(total, -d, True).astype(F32)
    own = (sums[0][0] + sums[0][1].astype(F32) + back[1] + back[2] + back[3] + back[4]).astype(BF)

    partner = swapped(own, "l")
    spread_rows = []
    for k in (1, 2, 3):
        spread_rows.append(turned(own, "y", k))
    partner, spread_rows = lax.optimization_barrier((partner, spread_rows))
    both = jnp.concatenate([own, partner], axis=1)
    first = lax.dynamic_index_in_dim(kv_weight, l, 0, keepdims=False)
    second = lax.dynamic_index_in_dim(kv_weight, 1 - l, 0, keepdims=False)
    input_grad = lax.dot_general(
        both,
        jnp.concatenate([first, second], axis=1),
        (((1,), (1,)), ((), ())),
        preferred_element_type=F32,
    ).astype(BF)

    rows = jnp.concatenate([own] + spread_rows, axis=0)
    norm = 1.0 / math.sqrt(tok * lax.axis_size(SEQ))
    weight_part = lax.dot_general(
        x_rows, rows, (((0,), (0,)), ((), ())), preferred_element_type=F32
    )
    weight_part = (weight_part * norm).reshape(16, 2, width // 32, hd)
    given = lax.dynamic_index_in_dim(weight_part, 1 - c, 1, keepdims=False)
    total = core_merged(c, weight_part, swapped(given.astype(BF), "c"))
    spread = lax.all_to_all(total, ("xh", "z"), split_axis=0, concat_axis=0, tiled=True)
    weight_grad = spread.astype(F32).sum(axis=0)
    return (query_grad, input_grad, weight_grad[None])


def solution(mesh):
    finer = Mesh(mesh.devices.reshape(4, 2, 8, 2, 2), ALL)
    placed = (
        P(SEQ, "l"),
        P(SEQ, None),
        P(SEQ, "l"),
        P(SEQ, None),
        P(None, "l", None),
        P(),
    )
    return jax.shard_map(
        local,
        mesh=finer,
        in_specs=placed,
        out_specs=(P(SEQ, "l"), P(SEQ, "l"), P("l", SEQ, None)),
        check_vma=False,
    )
```

```python
import math

import jax
import jax.numpy as jnp
from jax import lax
from jax.experimental import pallas as pl
from jax.experimental.pallas import tpu as pltpu
from jax.sharding import Mesh
from jax.sharding import PartitionSpec as P

WIN = 2048
SEQ = ("y", "xh", "z", "c")
ALL = ("y", "xh", "z", "c", "l")
PAIRS = 64
LINE = 8
BF = jnp.bfloat16
F32 = jnp.float32


def moved(value, steps, flip):
    routes = []
    for source in range(PAIRS):
        target = source + steps
        if not 0 <= target < PAIRS:
            continue
        turn = int(flip and source // LINE != target // LINE)
        for core in range(2):
            for side in range(2):
                routes.append(((source * 2 + core) * 2 + side, (target * 2 + core) * 2 + (side ^ turn)))
    return lax.ppermute(value, ALL, routes)


def swapped(value, axis):
    return lax.ppermute(value, axis, [(0, 1), (1, 0)])


def turned(value, axis, steps):
    count = lax.axis_size(axis)
    return lax.ppermute(value, axis, [(i, (i + steps) % count) for i in range(count)])


def columns(value, which, width):
    return lax.dynamic_slice_in_dim(value, which * width, width, 1)


def attention_kernel(
    side_ref,
    low_ref,
    query_ref,
    out_ref,
    own_ref,
    mine1,
    mine4,
    mine23,
    other1,
    other4,
    other23,
    near_ref,
    far_ref,
    query_grad_ref,
    given_ref,
    kept_ref,
    keys,
    values,
    queries,
    outs,
    probs,
    dprobs,
    tops,
    turned_grad,
):
    blocks, tok, hd = keys.shape
    heads = query_ref.shape[1] // hd
    inv_root = 1.0 / math.sqrt(hd)
    to_two = inv_root * math.log2(math.e)
    last = blocks - 1
    mine = {1: mine1, 4: mine4, 2: mine23.at[:tok], 3: mine23.at[tok:]}
    other = {1: other1, 4: other4, 2: other23.at[:tok], 3: other23.at[tok:]}
    for h in range(heads):
        queries[h * tok : (h + 1) * tok, :] = query_ref[:, h * hd : (h + 1) * hd]
        outs[h * tok : (h + 1) * tok, :] = out_ref[:, h * hd : (h + 1) * hd]

    @pl.when(side_ref[0] == 0)
    def _():
        for d in mine:
            keys[last - 2 * d] = mine[d][...]
            values[last - 2 * d] = other[d][...]

    @pl.when(side_ref[0] != 0)
    def _():
        for d in mine:
            keys[last - 2 * d] = other[d][...]
            values[last - 2 * d] = mine[d][...]

    keys[last] = own_ref[:, :hd]
    values[last] = own_ref[:, hd:]
    for place, ref, at in ((1, far_ref, 0), (3, far_ref, 1), (5, near_ref, 0), (7, near_ref, 1)):
        keys[place] = ref[at * tok : (at + 1) * tok, :hd]
        values[place] = ref[at * tok : (at + 1) * tok, hd:]

    along = (((1,), (1,)), ((), ()))
    down = (((0,), (0,)), ((), ()))
    low = low_ref[...]
    wide = heads * tok

    def first(block, carry, diagonal):
        top, mass, delta = carry
        row = lax.broadcasted_iota(jnp.int32, (tok, wide), 0)
        ok = row >= low - block * tok
        if diagonal:
            column = lax.broadcasted_iota(jnp.int32, (tok, wide), 1)
            ok = ok & (row <= (column & (tok - 1)))
        scores = lax.dot_general(keys[block], queries[...], along, preferred_element_type=F32)
        dprob = lax.dot_general(values[block], outs[...], along, preferred_element_type=F32)
        scores = jnp.where(ok, scores, -jnp.inf)
        here = jnp.max(scores, axis=0, keepdims=True)
        if not diagonal:
            here = jnp.maximum(here, top)
        prob = jnp.exp2((scores - here) * to_two)
        new_mass = jnp.sum(prob, axis=0, keepdims=True)
        new_delta = jnp.sum(prob * dprob, axis=0, keepdims=True)
        if not diagonal:
            fade = jnp.exp2((top - here) * to_two)
            new_mass = new_mass + mass * fade
            new_delta = new_delta + delta * fade
        probs[block] = prob
        dprobs[block] = dprob
        tops[block] = here
        return here, new_mass, new_delta

    carry = first(last, (None, None, None), True)
    carry = lax.fori_loop(0, last, lambda i, carry: first(i, carry, False), carry)
    top, mass, delta = carry
    inverse = 1.0 / mass
    delta = delta * inverse
    turned_grad[...] = jnp.zeros_like(turned_grad)

    def second(block, ref, at):
        factor = jnp.exp2((tops[block] - top) * to_two) * inverse
        prob = probs[block] * factor
        dscore = (prob * (dprobs[block] - delta)).astype(BF)
        key_grad = jnp.dot(dscore, queries[...], preferred_element_type=F32) * inv_root
        value_grad = jnp.dot(prob.astype(BF), outs[...], preferred_element_type=F32)
        ref[at, :, :hd] = key_grad.astype(BF)
        ref[at, :, hd:] = value_grad.astype(BF)
        turned_grad[...] += lax.dot_general(keys[block], dscore, down, preferred_element_type=F32)

    def odd(i, _):
        second(2 * i + 1, given_ref, i)
        return 0

    def even(i, _):
        second(2 * i, kept_ref, i)
        return 0

    lax.fori_loop(0, blocks // 2, odd, 0)
    lax.fori_loop(0, blocks // 2 + 1, even, 0)
    for h in range(heads):
        part = turned_grad[:, h * tok : (h + 1) * tok] * inv_root
        query_grad_ref[:, h * hd : (h + 1) * hd] = part.T.astype(BF)


def attention(side, low, query, out_grad, own, mine, other, near, far):
    tok, width = query.shape
    hd = own.shape[1] // 2
    heads = width // hd
    wide = heads * tok
    vmem = pl.BlockSpec(memory_space=pltpu.VMEM)
    work = 2 * 5 * wide * 9 * tok * hd
    return pl.pallas_call(
        attention_kernel,
        out_shape=(
            jax.ShapeDtypeStruct((tok, width), BF),
            jax.ShapeDtypeStruct((4, tok, 2 * hd), BF),
            jax.ShapeDtypeStruct((5, tok, 2 * hd), BF),
        ),
        in_specs=[pl.BlockSpec(memory_space=pltpu.SMEM)] + [vmem] * 12,
        out_specs=(vmem, vmem, vmem),
        scratch_shapes=[
            pltpu.VMEM((9, tok, hd), BF),
            pltpu.VMEM((9, tok, hd), BF),
            pltpu.VMEM((wide, hd), BF),
            pltpu.VMEM((wide, hd), BF),
            pltpu.VMEM((9, tok, wide), F32),
            pltpu.VMEM((9, tok, wide), F32),
            pltpu.VMEM((9, 1, wide), F32),
            pltpu.VMEM((hd, wide), F32),
        ],
        compiler_params=pltpu.CompilerParams(vmem_limit_bytes=48 * 1024 * 1024),
        cost_estimate=pl.CostEstimate(
            flops=work, transcendentals=wide * 9 * tok, bytes_accessed=8 * 1024 * 1024
        ),
        name="attention",
    )(side, low, query, out_grad, own, *mine, *other, near, far)


def merge_kernel(one_ref, two_ref, sum_ref):
    sum_ref[...] = (one_ref[...] + two_ref[...].astype(F32)).astype(sum_ref.dtype)


def merged(one, two):
    vmem = pl.BlockSpec(memory_space=pltpu.VMEM)
    return pl.pallas_call(
        merge_kernel,
        out_shape=jax.ShapeDtypeStruct(one.shape, BF),
        in_specs=[vmem, vmem],
        out_specs=vmem,
        compiler_params=pltpu.CompilerParams(vmem_limit_bytes=4 * 1024 * 1024),
        cost_estimate=pl.CostEstimate(flops=one.size, transcendentals=0, bytes_accessed=one.size * 8),
        name="merge",
    )(one, two)


def core_merge_kernel(core_ref, own_ref, arrived_ref, sum_ref):
    total = own_ref[:, core_ref[0]] + arrived_ref[...].astype(F32)
    sum_ref[...] = total.astype(BF)


def core_merged(core, own, arrived):
    vmem = pl.BlockSpec(memory_space=pltpu.VMEM)
    size = arrived.size
    return pl.pallas_call(
        core_merge_kernel,
        out_shape=jax.ShapeDtypeStruct(arrived.shape, BF),
        in_specs=[pl.BlockSpec(memory_space=pltpu.SMEM), vmem, vmem],
        out_specs=vmem,
        compiler_params=pltpu.CompilerParams(vmem_limit_bytes=8 * 1024 * 1024),
        cost_estimate=pl.CostEstimate(flops=size, transcendentals=0, bytes_accessed=size * 8),
        name="core_merge",
    )(core.reshape(1).astype(jnp.int32), own, arrived)


def local(query, key_value, out_grad, inputs_normed, kv_weight, segment_ids):
    tok = query.shape[0]
    hd = key_value.shape[1] // 2
    heads = query.shape[1] // hd
    y, _, z, c, l = (lax.axis_index(axis) for axis in ALL)
    seq_index = lax.axis_index(SEQ)

    def taken(distance):
        turn = (z + distance >= LINE).astype(jnp.int32)
        return columns(key_value, l ^ turn, hd)

    mine1 = moved(taken(1), 1, True)
    mine4 = moved(taken(4), 4, True)
    mine23 = moved(jnp.concatenate([columns(key_value, l, hd), mine1], axis=0), 2, False)
    other1 = swapped(mine1, "l")
    other4 = swapped(mine4, "l")
    other23 = swapped(mine23, "l")
    mine = {1: mine1, 4: mine4, 2: mine23[:tok], 3: mine23[tok:]}
    other = {1: other1, 4: other4, 2: other23[:tok], 3: other23[tok:]}
    blocks = {0: key_value}
    for d in (1, 2, 3, 4):
        blocks[d] = jnp.where(
            l == 0,
            jnp.concatenate([mine[d], other[d]], axis=1),
            jnp.concatenate([other[d], mine[d]], axis=1),
        )

    def crossing(low, high):
        return jnp.where(
            c == 0,
            jnp.concatenate([blocks[low + 1], blocks[low]], axis=0),
            jnp.concatenate([blocks[high + 1], blocks[high]], axis=0),
        )

    near = swapped(crossing(0, 1), "c")
    far = swapped(crossing(2, 3), "c")
    width = inputs_normed.shape[1] // 4
    x_parts = [columns(inputs_normed, y, width)]
    for k in (1, 2, 3):
        x_parts.append(turned(columns(inputs_normed, (y + k) % 4, width), "y", k))

    begin = seq_index * tok
    padded = jnp.concatenate([jnp.full((WIN,), -1, jnp.int32), segment_ids], axis=0)
    key_seg = lax.dynamic_slice_in_dim(padded, begin, WIN + tok, 0)
    query_seg = lax.dynamic_slice_in_dim(segment_ids, begin, tok, 0)
    before = jnp.sum((key_seg[:, None] < query_seg[None, :]).astype(jnp.int32), axis=0)
    low = jnp.maximum(before, 1 + jnp.arange(tok, dtype=jnp.int32))
    low = jnp.tile(low, heads)[None, :]
    query_grad, given, kept = attention(
        l.reshape(1).astype(jnp.int32),
        low,
        query,
        out_grad,
        key_value,
        (mine1, mine4, mine23),
        (other1, other4, other23),
        near,
        far,
    )
    arrived = swapped(given.reshape(4 * tok, 2 * hd), "c")
    x_rows = jnp.concatenate(x_parts, axis=0)

    def core_sum(d, which):
        def piece(j):
            if not 0 <= j < 4:
                return jnp.zeros((tok, hd), F32)
            rows = arrived[(3 - j) * tok : (4 - j) * tok]
            return columns(rows, which, hd).astype(F32)

        return columns(kept[4 - d], which, hd).astype(F32) + jnp.where(c == 0, piece(d), piece(d - 1))

    back = {}
    sums = {}
    for d in (4, 3, 2, 1, 0):
        side = l ^ (z < d).astype(jnp.int32)
        got = swapped(core_sum(d, 1 - side).astype(BF), "l")
        sums[d] = (core_sum(d, side), got)
    for d in (3, 4, 2, 1):
        total = merged(*sums[d])
        back[d] = moved(total, -d, True).astype(F32)
    own = (sums[0][0] + sums[0][1].astype(F32) + back[1] + back[2] + back[3] + back[4]).astype(BF)

    partner = swapped(own, "l")
    spread_rows = []
    for k in (1, 2, 3):
        spread_rows.append(turned(own, "y", k))
    partner, spread_rows = lax.optimization_barrier((partner, spread_rows))
    both = jnp.concatenate([own, partner], axis=1)
    first = lax.dynamic_index_in_dim(kv_weight, l, 0, keepdims=False)
    second = lax.dynamic_index_in_dim(kv_weight, 1 - l, 0, keepdims=False)
    input_grad = lax.dot_general(
        both,
        jnp.concatenate([first, second], axis=1),
        (((1,), (1,)), ((), ())),
        preferred_element_type=F32,
    ).astype(BF)

    rows = jnp.concatenate([own] + spread_rows, axis=0)
    norm = 1.0 / math.sqrt(tok * lax.axis_size(SEQ))
    weight_part = lax.dot_general(
        x_rows, rows, (((0,), (0,)), ((), ())), preferred_element_type=F32
    )
    weight_part = (weight_part * norm).reshape(16, 2, width // 32, hd)
    given = lax.dynamic_index_in_dim(weight_part, 1 - c, 1, keepdims=False)
    total = core_merged(c, weight_part, swapped(given.astype(BF), "c"))
    spread = lax.all_to_all(total, ("xh", "z"), split_axis=0, concat_axis=0, tiled=True)
    weight_grad = spread.astype(F32).sum(axis=0)
    return (query_grad, input_grad, weight_grad[None])


def solution(mesh):
    finer = Mesh(mesh.devices.reshape(4, 2, 8, 2, 2), ALL)
    placed = (
        P(SEQ, "l"),
        P(SEQ, None),
        P(SEQ, "l"),
        P(SEQ, None),
        P(None, "l", None),
        P(),
    )
    return jax.shard_map(
        local,
        mesh=finer,
        in_specs=placed,
        out_specs=(P(SEQ, "l"), P(SEQ, "l"), P("l", SEQ, None)),
        check_vma=False,
    )
```

```python
import math

import jax
import jax.numpy as jnp
from jax import lax
from jax.experimental import pallas as pl
from jax.experimental.pallas import tpu as pltpu
from jax.sharding import Mesh
from jax.sharding import PartitionSpec as P

WIN = 2048
SEQ = ("y", "xh", "z", "c")
ALL = ("y", "xh", "z", "c", "l")
PAIRS = 64
LINE = 8
BF = jnp.bfloat16
F32 = jnp.float32


def moved(value, steps, flip):
    routes = []
    for source in range(PAIRS):
        target = source + steps
        if not 0 <= target < PAIRS:
            continue
        turn = int(flip and source // LINE != target // LINE)
        for core in range(2):
            for side in range(2):
                routes.append(((source * 2 + core) * 2 + side, (target * 2 + core) * 2 + (side ^ turn)))
    return lax.ppermute(value, ALL, routes)


def swapped(value, axis):
    return lax.ppermute(value, axis, [(0, 1), (1, 0)])


def turned(value, axis, steps):
    count = lax.axis_size(axis)
    return lax.ppermute(value, axis, [(i, (i + steps) % count) for i in range(count)])


def columns(value, which, width):
    return lax.dynamic_slice_in_dim(value, which * width, width, 1)


def attention_kernel(
    side_ref,
    low_ref,
    query_ref,
    out_ref,
    own_ref,
    mine1,
    mine4,
    mine23,
    other1,
    other4,
    other23,
    near_ref,
    far_ref,
    query_grad_ref,
    given_ref,
    kept_ref,
    keys,
    values,
    queries,
    outs,
    probs,
    dprobs,
    tops,
    turned_grad,
):
    blocks, tok, hd = keys.shape
    heads = query_ref.shape[1] // hd
    inv_root = 1.0 / math.sqrt(hd)
    to_two = inv_root * math.log2(math.e)
    last = blocks - 1
    mine = {1: mine1, 4: mine4, 2: mine23.at[:tok], 3: mine23.at[tok:]}
    other = {1: other1, 4: other4, 2: other23.at[:tok], 3: other23.at[tok:]}
    for h in range(heads):
        queries[h * tok : (h + 1) * tok, :] = query_ref[:, h * hd : (h + 1) * hd]
        outs[h * tok : (h + 1) * tok, :] = out_ref[:, h * hd : (h + 1) * hd]

    for at, distances in ((0, (2, 3, 4)), (1, (1,))):

        @pl.when(side_ref[at] == 0)
        def _():
            for d in distances:
                keys[last - 2 * d] = mine[d][...]
                values[last - 2 * d] = other[d][...]

        @pl.when(side_ref[at] != 0)
        def _():
            for d in distances:
                keys[last - 2 * d] = other[d][...]
                values[last - 2 * d] = mine[d][...]

    keys[last] = own_ref[:, :hd]
    values[last] = own_ref[:, hd:]
    for place, ref, at in ((1, far_ref, 0), (3, far_ref, 1), (5, near_ref, 0), (7, near_ref, 1)):
        keys[place] = ref[at * tok : (at + 1) * tok, :hd]
        values[place] = ref[at * tok : (at + 1) * tok, hd:]

    along = (((1,), (1,)), ((), ()))
    down = (((0,), (0,)), ((), ()))
    low = low_ref[...]
    wide = heads * tok

    def first(block, carry, diagonal):
        top, mass, delta = carry
        row = lax.broadcasted_iota(jnp.int32, (tok, wide), 0)
        ok = row >= low - block * tok
        if diagonal:
            column = lax.broadcasted_iota(jnp.int32, (tok, wide), 1)
            ok = ok & (row <= (column & (tok - 1)))
        scores = lax.dot_general(keys[block], queries[...], along, preferred_element_type=F32)
        dprob = lax.dot_general(values[block], outs[...], along, preferred_element_type=F32)
        scores = jnp.where(ok, scores, -jnp.inf)
        here = jnp.max(scores, axis=0, keepdims=True)
        if not diagonal:
            here = jnp.maximum(here, top)
        prob = jnp.exp2((scores - here) * to_two)
        new_mass = jnp.sum(prob, axis=0, keepdims=True)
        new_delta = jnp.sum(prob * dprob, axis=0, keepdims=True)
        if not diagonal:
            fade = jnp.exp2((top - here) * to_two)
            new_mass = new_mass + mass * fade
            new_delta = new_delta + delta * fade
        probs[block] = prob
        dprobs[block] = dprob
        tops[block] = here
        return here, new_mass, new_delta

    carry = first(last, (None, None, None), True)
    carry = lax.fori_loop(0, last, lambda i, carry: first(i, carry, False), carry)
    top, mass, delta = carry
    inverse = 1.0 / mass
    delta = delta * inverse
    turned_grad[...] = jnp.zeros_like(turned_grad)

    def second(block, ref, at):
        factor = jnp.exp2((tops[block] - top) * to_two) * inverse
        prob = probs[block] * factor
        dscore = (prob * (dprobs[block] - delta)).astype(BF)
        key_grad = jnp.dot(dscore, queries[...], preferred_element_type=F32) * inv_root
        value_grad = jnp.dot(prob.astype(BF), outs[...], preferred_element_type=F32)
        ref[at, :, :hd] = key_grad.astype(BF)
        ref[at, :, hd:] = value_grad.astype(BF)
        turned_grad[...] += lax.dot_general(keys[block], dscore, down, preferred_element_type=F32)

    def odd(i, _):
        second(2 * i + 1, given_ref, i)
        return 0

    def even(i, _):
        second(2 * i, kept_ref, i)
        return 0

    lax.fori_loop(0, blocks // 2, odd, 0)
    lax.fori_loop(0, blocks // 2 + 1, even, 0)
    for h in range(heads):
        part = turned_grad[:, h * tok : (h + 1) * tok] * inv_root
        query_grad_ref[:, h * hd : (h + 1) * hd] = part.T.astype(BF)


def attention(side, low, query, out_grad, own, mine, other, near, far):
    tok, width = query.shape
    hd = own.shape[1] // 2
    heads = width // hd
    wide = heads * tok
    vmem = pl.BlockSpec(memory_space=pltpu.VMEM)
    work = 2 * 5 * wide * 9 * tok * hd
    return pl.pallas_call(
        attention_kernel,
        out_shape=(
            jax.ShapeDtypeStruct((tok, width), BF),
            jax.ShapeDtypeStruct((4, tok, 2 * hd), BF),
            jax.ShapeDtypeStruct((5, tok, 2 * hd), BF),
        ),
        in_specs=[pl.BlockSpec(memory_space=pltpu.SMEM)] + [vmem] * 12,
        out_specs=(vmem, vmem, vmem),
        scratch_shapes=[
            pltpu.VMEM((9, tok, hd), BF),
            pltpu.VMEM((9, tok, hd), BF),
            pltpu.VMEM((wide, hd), BF),
            pltpu.VMEM((wide, hd), BF),
            pltpu.VMEM((9, tok, wide), F32),
            pltpu.VMEM((9, tok, wide), F32),
            pltpu.VMEM((9, 1, wide), F32),
            pltpu.VMEM((hd, wide), F32),
        ],
        compiler_params=pltpu.CompilerParams(vmem_limit_bytes=48 * 1024 * 1024),
        cost_estimate=pl.CostEstimate(
            flops=work, transcendentals=wide * 9 * tok, bytes_accessed=8 * 1024 * 1024
        ),
        name="attention",
    )(side, low, query, out_grad, own, *mine, *other, near, far)


def merge_kernel(one_ref, two_ref, sum_ref):
    sum_ref[...] = (one_ref[...] + two_ref[...].astype(F32)).astype(sum_ref.dtype)


def merged(one, two):
    vmem = pl.BlockSpec(memory_space=pltpu.VMEM)
    return pl.pallas_call(
        merge_kernel,
        out_shape=jax.ShapeDtypeStruct(one.shape, BF),
        in_specs=[vmem, vmem],
        out_specs=vmem,
        compiler_params=pltpu.CompilerParams(vmem_limit_bytes=4 * 1024 * 1024),
        cost_estimate=pl.CostEstimate(flops=one.size, transcendentals=0, bytes_accessed=one.size * 8),
        name="merge",
    )(one, two)


def core_merge_kernel(core_ref, own_ref, arrived_ref, sum_ref):
    total = own_ref[:, core_ref[0]] + arrived_ref[...].astype(F32)
    sum_ref[...] = total.astype(BF)


def core_merged(core, own, arrived):
    vmem = pl.BlockSpec(memory_space=pltpu.VMEM)
    size = arrived.size
    return pl.pallas_call(
        core_merge_kernel,
        out_shape=jax.ShapeDtypeStruct(arrived.shape, BF),
        in_specs=[pl.BlockSpec(memory_space=pltpu.SMEM), vmem, vmem],
        out_specs=vmem,
        compiler_params=pltpu.CompilerParams(vmem_limit_bytes=8 * 1024 * 1024),
        cost_estimate=pl.CostEstimate(flops=size, transcendentals=0, bytes_accessed=size * 8),
        name="core_merge",
    )(core.reshape(1).astype(jnp.int32), own, arrived)


def local(query, key_value, out_grad, inputs_normed, kv_weight, segment_ids):
    tok = query.shape[0]
    hd = key_value.shape[1] // 2
    heads = query.shape[1] // hd
    y, _, z, c, l = (lax.axis_index(axis) for axis in ALL)
    seq_index = lax.axis_index(SEQ)

    def taken(distance):
        turn = (z + distance >= LINE).astype(jnp.int32)
        return columns(key_value, l ^ turn, hd)

    ahead = (z >= LINE - 2).astype(jnp.int32)
    ahead_next = ((z + 1) % LINE >= LINE - 2).astype(jnp.int32)
    turn = (z + 1 >= LINE).astype(jnp.int32)
    mine1 = moved(columns(key_value, l ^ turn ^ ahead_next, hd), 1, True)
    mine4 = moved(taken(4), 4, True)
    couple = jnp.concatenate([taken(2), mine1], axis=0)
    mine23 = moved(couple, 2, True)
    other1 = swapped(mine1, "l")
    other4 = swapped(mine4, "l")
    other23 = swapped(mine23, "l")
    mine = {1: mine1, 4: mine4, 2: mine23[:tok], 3: mine23[tok:]}
    other = {1: other1, 4: other4, 2: other23[:tok], 3: other23[tok:]}
    blocks = {0: key_value}
    for d in (1, 2, 3, 4):
        blocks[d] = jnp.where(
            (l ^ ahead if d == 1 else l) == 0,
            jnp.concatenate([mine[d], other[d]], axis=1),
            jnp.concatenate([other[d], mine[d]], axis=1),
        )

    def crossing(low, high):
        return jnp.where(
            c == 0,
            jnp.concatenate([blocks[low + 1], blocks[low]], axis=0),
            jnp.concatenate([blocks[high + 1], blocks[high]], axis=0),
        )

    near = swapped(crossing(0, 1), "c")
    far = swapped(crossing(2, 3), "c")
    width = inputs_normed.shape[1] // 4
    inputs, _ = lax.optimization_barrier((inputs_normed, couple))
    x_parts = [columns(inputs, y, width)]
    for k in (1, 2, 3):
        x_parts.append(turned(columns(inputs, (y + k) % 4, width), "y", k))

    begin = seq_index * tok
    padded = jnp.concatenate([jnp.full((WIN,), -1, jnp.int32), segment_ids], axis=0)
    key_seg = lax.dynamic_slice_in_dim(padded, begin, WIN + tok, 0)
    query_seg = lax.dynamic_slice_in_dim(segment_ids, begin, tok, 0)
    before = jnp.sum((key_seg[:, None] < query_seg[None, :]).astype(jnp.int32), axis=0)
    low = jnp.maximum(before, 1 + jnp.arange(tok, dtype=jnp.int32))
    low = jnp.tile(low, heads)[None, :]
    query_grad, given, kept = attention(
        jnp.stack([l, l ^ ahead]).astype(jnp.int32),
        low,
        query,
        out_grad,
        key_value,
        (mine1, mine4, mine23),
        (other1, other4, other23),
        near,
        far,
    )
    arrived = swapped(given.reshape(4 * tok, 2 * hd), "c")
    x_rows = jnp.concatenate(x_parts, axis=0)

    def core_sum(d, which):
        def piece(j):
            if not 0 <= j < 4:
                return jnp.zeros((tok, hd), F32)
            rows = arrived[(3 - j) * tok : (4 - j) * tok]
            return columns(rows, which, hd).astype(F32)

        return columns(kept[4 - d], which, hd).astype(F32) + jnp.where(c == 0, piece(d), piece(d - 1))

    back = {}
    sums = {}
    for d in (4, 3, 2, 1, 0):
        side = l ^ (z < d).astype(jnp.int32)
        got = swapped(core_sum(d, 1 - side).astype(BF), "l")
        sums[d] = (core_sum(d, side), got)
    for d in (3, 4, 2, 1):
        total = merged(*sums[d])
        back[d] = moved(total, -d, True).astype(F32)
    own = (sums[0][0] + sums[0][1].astype(F32) + back[1] + back[2] + back[3] + back[4]).astype(BF)

    partner = swapped(own, "l")
    spread_rows = []
    for k in (1, 2, 3):
        spread_rows.append(turned(own, "y", k))
    partner, spread_rows = lax.optimization_barrier((partner, spread_rows))
    both = jnp.concatenate([own, partner], axis=1)
    first = lax.dynamic_index_in_dim(kv_weight, l, 0, keepdims=False)
    second = lax.dynamic_index_in_dim(kv_weight, 1 - l, 0, keepdims=False)
    input_grad = lax.dot_general(
        both,
        jnp.concatenate([first, second], axis=1),
        (((1,), (1,)), ((), ())),
        preferred_element_type=F32,
    ).astype(BF)

    rows = jnp.concatenate([own] + spread_rows, axis=0)
    norm = 1.0 / math.sqrt(tok * lax.axis_size(SEQ))
    weight_part = lax.dot_general(
        x_rows, rows, (((0,), (0,)), ((), ())), preferred_element_type=F32
    )
    weight_part = (weight_part * norm).reshape(16, 2, width // 32, hd)
    given = lax.dynamic_index_in_dim(weight_part, 1 - c, 1, keepdims=False)
    total = core_merged(c, weight_part, swapped(given.astype(BF), "c"))
    spread = lax.all_to_all(total, ("xh", "z"), split_axis=0, concat_axis=0, tiled=True)
    weight_grad = spread.astype(F32).sum(axis=0)
    return (query_grad, input_grad, weight_grad[None])


def solution(mesh):
    finer = Mesh(mesh.devices.reshape(4, 2, 8, 2, 2), ALL)
    placed = (
        P(SEQ, "l"),
        P(SEQ, None),
        P(SEQ, "l"),
        P(SEQ, None),
        P(None, "l", None),
        P(),
    )
    return jax.shard_map(
        local,
        mesh=finer,
        in_specs=placed,
        out_specs=(P(SEQ, "l"), P(SEQ, "l"), P("l", SEQ, None)),
        check_vma=False,
    )
```
